32 devices in a mesh: parts: 2 (over y), modes: 16 (over z, x, core).
Axes of the slice: x: 2, y: 2, z: 4, core: 2. Of those that a mesh axis runs over, the one named last changes fastest.
Arguments:
- stem: bfloat16 [2, 16, 64, 32, 512], P(None, 'modes', None, None, 'parts'), parts along dimension 4, may hold values from -6 to 6
- branch_one: bfloat16 [2, 1024, 1024], replicated, may hold values from -0.125 to 0.125
- branch_two: bfloat16 [2, 1024, 1024], replicated, may hold values from -0.125 to 0.125
- branch_three: bfloat16 [2, 2, 16, 512, 512], P(None, None, 'modes'), may hold values from -0.0625 to 0.0625
- leg_orders: int32 [2, 10], replicated, may hold values from 0 to 9, each once within a row
- slice_pick: int32 [32], P('parts'), parts along dimension 0, may hold values from 0 to 1
Outputs:
- contracted: bfloat16 [1024, 2, 2, 2, 256], P(('parts', 'modes')), parts along dimension 0
The draws below stay inside these ranges and needn't reach their ends.
There are 2 independent parts, one for each index of `parts`. The reference program is written for one: setup_inputs(seed, part) draws one part's arguments, and reference() takes and returns one part's arrays. A program takes and returns all parts, laid end to end along the dimension named above; an argument that names none is the same for every part. Nothing has to cross between parts.
Inputs may be any that keep to these rules, and one draw needn't show every extreme that they name: `leg_orders`: each row names every input leg bit once.
All inputs are finite; a program needn't handle non-finite values.
Results may differ from the reference program's by a relative error of at most 0.008.
Values may be sent and summed in bfloat16 or wider, within the bound.
A program may use at most 128 MiB of HBM per device.

```python
import jax
import jax.numpy as jnp

LEGS = 10
C = 1024
OUTW = 512
SLICES = 2
ROWS_DEV = 2
L = 256
E = 64
H = 32
N_MODES = 16


def with_ends(values, own_key, low, top_value):
    shape = values.shape
    place = [jax.random.randint(jax.random.fold_in(own_key, axis), (), 0, shape[axis]) for axis in range(len(shape))]
    values = values.at[tuple(place)].set(low)
    longest = shape.index(max(shape))
    place[longest] = (place[longest] + 1) % shape[longest]
    return values.at[tuple(place)].set(top_value)


def raised(drawn, key, source, target, blocks, factor):
    def block_of(dim):
        return (jnp.arange(drawn.shape[dim]) // (drawn.shape[dim] // blocks)).reshape((-1,) + (1,) * (drawn.ndim - 1 - dim))

    one_side = jax.random.permutation(key, blocks)[block_of(target)]
    other_side = (block_of(target) + blocks // 2) % blocks
    return jnp.where((block_of(source) == one_side) | (block_of(source) == other_side), factor * drawn, drawn)


def levels(stream_key, extent, shards, low, largest):
    def one(axis_at, parts):
        heights = jax.random.uniform(jax.random.fold_in(jax.random.fold_in(stream_key, 6), axis_at), (parts,), jnp.float32, low / len(shards), largest / len(shards))
        return jnp.repeat(jnp.exp(heights), extent[axis_at] // parts).reshape((-1,) + (1,) * (len(extent) - axis_at - 1))

    factor_of = one(*shards[0])
    for cut in shards[1:]:
        factor_of = factor_of * one(*cut)
    return factor_of


def bell_draw(rng, shape, deviation, bound, shards=(), kind=jnp.bfloat16):
    gain = levels(rng, shape, shards, -0.22, 0.18) if shards else 1.0
    drawn = jax.random.normal(rng, shape, jnp.float32) * deviation * gain
    return jnp.minimum(jnp.maximum(drawn, -bound), bound).astype(kind)


def gaussian_with(key, dims, width, most, pieces, heavy, kind=jnp.bfloat16):
    values = width * jax.random.normal(key, dims, jnp.float32)
    if pieces:
        values = values * levels(key, dims, pieces, -0.22, 0.18)
    return jnp.clip(raised(values, jax.random.fold_in(key, 3), *heavy), -most, most).astype(kind)


def setup_inputs(seed: int = 0, part: int = 0) -> dict:
    splits = jax.random.split(jax.random.key(seed), 7)
    own_keys = jax.random.split(jax.random.fold_in(splits[6], part), 7)
    stem = bell_draw(own_keys[0], (2, N_MODES, E, H, L), 1.0, 6.0, ((1, 16),))
    branch_one = bell_draw(splits[1], (2, C, C), (2 * C) ** -0.5, 0.125)
    branch_two = bell_draw(splits[2], (2, C, C), (2 * C) ** -0.5, 0.125)
    branch_three = gaussian_with(splits[3], (SLICES, 2, N_MODES, OUTW, C // 2), (N_MODES * C) ** -0.5, 0.0625, ((2, 16),), (2, 3, 16, 2.0))
    leg_orders = jax.vmap(lambda own: jax.random.permutation(own, LEGS))(jax.random.split(splits[4], 2)).reshape((2, LEGS)).astype(jnp.int32)
    slice_pick = with_ends(jax.random.randint(own_keys[5], (N_MODES,), 0, SLICES), jax.random.fold_in(own_keys[5], 1), 0, SLICES - 1).astype(jnp.int32)
    return dict(stem=stem, branch_one=branch_one, branch_two=branch_two, branch_three=branch_three, leg_orders=leg_orders, slice_pick=slice_pick)


def leg_index(order, leg_width):
    positions = jnp.arange(leg_width, dtype=jnp.int32)
    shifts = jnp.arange(order.shape[0], dtype=jnp.int32)
    digits = jnp.right_shift(positions[:, None], shifts[None, :]) % 2
    placed = jnp.left_shift(digits, order[None, :].astype(jnp.int32))
    return jnp.sum(placed, axis=1).astype(jnp.int32)


def complex_apply(weight, values):
    real_part = weight[0]
    imag_part = weight[1]
    block_matrix = jnp.concatenate([jnp.concatenate([real_part, -imag_part], axis=1), jnp.concatenate([imag_part, real_part], axis=1)], axis=0)
    stacked = values.reshape(2 * values.shape[1], values.shape[2])
    result = jnp.dot(block_matrix, stacked, preferred_element_type=jnp.float32)
    return result.reshape(2, weight.shape[1], values.shape[2])


def reference(stem, branch_one, branch_two, branch_three, leg_orders, slice_pick):
    groups = N_MODES
    half_width = C // 2
    quarter = groups // 4
    columns = ROWS_DEV * groups * L
    values = stem.reshape(2, C, columns)
    weight_one = jnp.take(branch_one, leg_index(leg_orders[0], C), axis=2)
    after_first = complex_apply(weight_one, values).astype(jnp.bfloat16)
    after_first = after_first.reshape(2, 2, half_width, 2, quarter, 2, ROWS_DEV, L)
    second_in = after_first.transpose(0, 3, 2, 1, 4, 5, 6, 7).reshape(2, C, columns)
    weight_two = jnp.take(branch_two, leg_index(leg_orders[1], C), axis=2)
    after_second = complex_apply(weight_two, second_in).astype(jnp.bfloat16)
    after_second = after_second.reshape(2, 2, half_width, 2, quarter, 2, ROWS_DEV, L)
    third_in = after_second.transpose(0, 3, 4, 6, 2, 1, 5, 7).reshape(2, groups * half_width, 4 * L)
    split_ids = jnp.arange(groups, dtype=jnp.int32)
    picked = branch_three[slice_pick.astype(jnp.int32), :, split_ids]
    chosen = picked.transpose(1, 0, 2, 3)
    weight_three = chosen.transpose(0, 2, 1, 3).reshape(2, OUTW, groups * half_width)
    after_third = complex_apply(weight_three, third_in)
    return after_third.reshape(2, OUTW, 2, 2, L).transpose(1, 0, 2, 3, 4).astype(jnp.bfloat16)
```

```python
import jax
import jax.numpy as jnp
from jax import lax
from jax.experimental import pallas as pl
from jax.experimental.pallas import tpu as pltpu
from jax.sharding import PartitionSpec as P

TILES = 4
CHUNKS = 4
MESH = pl.DeviceIdType.MESH


def turn_columns(order, branch, out, onehot):
    width = branch.shape[1]

    @pl.when(pl.program_id(0) == 0)
    def _():
        positions = lax.broadcasted_iota(jnp.int32, (1, width), 1)
        source = jnp.zeros((1, width), jnp.int32)
        for bit in range(order.shape[0]):
            source += jnp.left_shift(jnp.right_shift(positions, bit) & 1, order[bit])
        rows = lax.broadcasted_iota(jnp.int32, (width, width), 0)
        onehot[...] = jnp.where(rows == source, 1.0, 0.0).astype(onehot.dtype)

    out[...] = jnp.dot(
        branch[...], onehot[...], preferred_element_type=jnp.float32
    ).astype(out.dtype)


def turned(branch, order, name):
    width = branch.shape[2]
    flat = branch.reshape(-1, width)
    tile = flat.shape[0] // 8
    out = pl.pallas_call(
        turn_columns,
        name=name,
        grid=(8,),
        out_shape=jax.ShapeDtypeStruct(flat.shape, flat.dtype),
        in_specs=[
            pl.BlockSpec(memory_space=pltpu.SMEM),
            pl.BlockSpec((tile, width), lambda i: (i, 0)),
        ],
        out_specs=pl.BlockSpec((tile, width), lambda i: (i, 0)),
        scratch_shapes=[pltpu.VMEM((width, width), flat.dtype)],
        compiler_params=pltpu.CompilerParams(vmem_limit_bytes=58 * 2**20),
        cost_estimate=pl.CostEstimate(
            flops=2 * flat.shape[0] * width * width,
            bytes_accessed=4 * flat.size,
            transcendentals=0,
        ),
    )(order, flat)
    return out.reshape(branch.shape)


def complex_tile(w, values):
    half = values.shape[1] // 2
    p = jnp.dot(w[0], values, preferred_element_type=jnp.float32)
    q = jnp.dot(w[1], values, preferred_element_type=jnp.float32)
    real = p[:, :half] - q[:, half:]
    imag = p[:, half:] + q[:, :half]
    return real.astype(jnp.bfloat16), imag.astype(jnp.bfloat16)


def two_branches(x_hbm, w1_hbm, w2_hbm, out, x, w1, w2, mid, sems):
    width = x.shape[0]
    half = width // 2
    tile = width // TILES
    lanes = x.shape[1] // 8
    copies = [pltpu.make_async_copy(x_hbm, x, sems.at[0])]
    for which, (source, target) in enumerate(((w1_hbm, w1), (w2_hbm, w2))):
        for i in range(TILES):
            rows = pl.ds(i * tile, tile)
            copies.append(
                pltpu.make_async_copy(
                    source.at[:, rows, :], target.at[:, rows, :], sems.at[1 + which * TILES + i]
                )
            )
    for copy in copies:
        copy.start()
    copies[0].wait()
    for i in range(TILES):
        copies[1 + i].wait()
        t, c = divmod(i * tile, half)
        parts = complex_tile(w1[:, i * tile : (i + 1) * tile, :], x[...])
        for r in range(2):
            for a in range(2):
                at = (2 * r + t) * 2 * lanes
                mid[a * half + c : a * half + c + tile, at : at + 2 * lanes] = parts[r][
                    :, a * 2 * lanes : (a + 1) * 2 * lanes
                ]
    for i in range(TILES):
        copies[1 + TILES + i].wait()
        u, c = divmod(i * tile, half)
        parts = complex_tile(w2[:, i * tile : (i + 1) * tile, :], mid[...])
        for r in range(2):
            for td in range(4):
                at = (2 * r + u) * lanes
                out[td, c : c + tile, at : at + lanes] = parts[r][:, td * lanes : (td + 1) * lanes]


def third_branch(place, wa, wb, wc, wd, values, out):
    k2 = place[0]
    k0 = place[1]
    half = values.shape[2] // 2
    p = q = None
    for w, t, d in ((wa, k2, k0), (wb, 1 - k2, k0), (wc, k2, 1 - k0), (wd, 1 - k2, 1 - k0)):
        block = values[2 * t + d]
        pp = jnp.dot(w[0], block, preferred_element_type=jnp.float32)
        qq = jnp.dot(w[1], block, preferred_element_type=jnp.float32)
        p = pp if p is None else p + pp
        q = qq if q is None else q + qq
    out[:, :half] = (p[:, :half] - q[:, half:]).astype(out.dtype)
    out[:, half:] = (p[:, half:] + q[:, :half]).astype(out.dtype)


def by_columns(stem, branch_one, branch_two, branch_three, leg_orders, slice_pick):
    groups = lax.axis_size("modes")
    me = lax.axis_index("modes")
    rest = groups // 8
    entries, lanes = stem.shape[2], stem.shape[4] // 2
    k2 = (me // (2 * rest)) % 2
    quarter = me // (2 * rest)
    k0 = me % 2

    cut = stem.reshape(2, entries, 2, 2, rest, 2, 2, 2, lanes)
    cut = cut.transpose(3, 7, 4, 5, 1, 0, 2, 6, 8).reshape(groups, entries, 8 * lanes)
    pick = lax.dynamic_index_in_dim(slice_pick, me, 0, keepdims=False)
    own = lax.dynamic_index_in_dim(branch_three, pick, 0, keepdims=False)[:, 0]
    q = 2 * rest
    middle = [(q + i, 2 * q + i) for i in range(q)]
    middle += [(b, a) for a, b in middle]
    outer = [(i, i ^ q) for i in range(groups)] if q & (q - 1) == 0 else [
        (i, i + q if (i // q) % 2 == 0 else i - q) for i in range(groups)
    ]
    cores = [(i, i ^ 1) for i in range(groups)]
    crossed = lax.ppermute(own, "modes", middle)
    w1 = turned(branch_one, leg_orders[0], "turn_one")
    cut, crossed, w1, branch_two = lax.optimization_barrier((cut, crossed, w1, branch_two))
    arrived = lax.all_to_all(cut, "modes", split_axis=0, concat_axis=0, tiled=True)
    x = arrived.reshape(groups * entries, 8 * lanes)
    w2 = turned(branch_two, leg_orders[1], "turn_two")
    crossed, w2 = lax.optimization_barrier((crossed, w2))
    inner = (quarter == 1) | (quarter == 2)
    wa = jnp.where(inner, crossed, own)
    wb = lax.ppermute(wa, "modes", outer)
    wc = lax.ppermute(wa, "modes", cores)
    wd = lax.ppermute(wb, "modes", cores)

    width = w1.shape[1]
    half = width // 2
    any_spec = pl.BlockSpec(memory_space=pl.ANY)
    vmem = pl.BlockSpec(memory_space=pltpu.VMEM)
    values = pl.pallas_call(
        two_branches,
        name="two_branches",
        out_shape=jax.ShapeDtypeStruct((4, half, 4 * lanes), jnp.bfloat16),
        in_specs=[any_spec] * 3,
        out_specs=vmem,
        scratch_shapes=[
            pltpu.VMEM(x.shape, x.dtype),
            pltpu.VMEM(w1.shape, w1.dtype),
            pltpu.VMEM(w2.shape, w2.dtype),
            pltpu.VMEM((width, 8 * lanes), jnp.bfloat16),
            pltpu.SemaphoreType.DMA((1 + 2 * TILES,)),
        ],
        compiler_params=pltpu.CompilerParams(vmem_limit_bytes=58 * 2**20),
        cost_estimate=pl.CostEstimate(
            flops=8 * width * width * 8 * lanes, bytes_accessed=12 * 2**20, transcendentals=0
        ),
    )(x, w1, w2)

    out_width = own.shape[1]
    partial = pl.pallas_call(
        third_branch,
        name="third_branch",
        out_shape=jax.ShapeDtypeStruct((out_width, 4 * lanes), jnp.bfloat16),
        in_specs=[pl.BlockSpec(memory_space=pltpu.SMEM)] + [vmem] * 5,
        out_specs=vmem,
        compiler_params=pltpu.CompilerParams(vmem_limit_bytes=24 * 2**20),
        cost_estimate=pl.CostEstimate(
            flops=16 * out_width * half * 4 * lanes, bytes_accessed=7 * 2**20, transcendentals=0
        ),
    )(jnp.stack([k2, k0]).astype(jnp.int32), wa, wb, wc, wd, values)

    pieces = lax.all_to_all(partial, "modes", split_axis=0, concat_axis=0, tiled=True)
    mine = out_width // groups
    pieces = pieces.reshape(2, 2, rest, 2, mine, 2, 2, lanes).astype(jnp.float32)
    summed = jnp.sum(pieces, axis=(0, 2)).astype(jnp.bfloat16)
    return summed.transpose(2, 3, 4, 1, 0, 5).reshape(mine, 2, 2, 2, 2 * lanes)


def spread(order, which, start, onehot):
    rows, width = onehot.shape
    positions = start + lax.broadcasted_iota(jnp.int32, (1, width), 1)
    source = jnp.zeros((1, width), jnp.int32)
    for bit in range(order.shape[1]):
        source += jnp.left_shift(jnp.right_shift(positions, bit) & 1, order[which, bit])
    tile = 256

    @pl.loop(0, rows // tile)
    def _(i):
        at = i * tile + lax.broadcasted_iota(jnp.int32, (tile, width), 0)
        onehot[pl.ds(pl.multiple_of(i * tile, tile), tile), :] = jnp.where(
            at == source, 1.0, 0.0
        ).astype(onehot.dtype)


def turn(branch, onehot, w):
    rows, width = branch.shape[1], onehot.shape[1]
    tile = 256

    @pl.loop(0, rows // tile)
    def _(i):
        at = pl.ds(pl.multiple_of(i * tile, tile), tile)
        real = jnp.dot(branch[0, at, :], onehot[...], preferred_element_type=jnp.float32)
        real = real.astype(w.dtype)
        w[0, at, :width] = real
        w[1, at, width:] = real
        imag = jnp.dot(branch[1, at, :], onehot[...], preferred_element_type=jnp.float32)
        w[0, at, width:] = (-imag).astype(w.dtype)
        w[1, at, :width] = imag.astype(w.dtype)


def blocks(w):
    rows = w.shape[1] * w.shape[2]
    real = w[0].astype(jnp.float32).reshape(rows, w.shape[3])
    imag = w[1].astype(jnp.float32).reshape(rows, w.shape[3])
    return jnp.concatenate(
        [jnp.concatenate([real, -imag], axis=1), jnp.concatenate([imag, real], axis=1)], axis=0
    ).astype(w.dtype)


def contraction(
    order, pick, stem, b1, b2, w3, out,
    xin, turned_x, cut, x, raw1, raw2, onehot, w1, w2, mid, y2, raw3, own3, relay3, cross3, acc,
    keeps, sends, gots, load_sem, x_send, x_recv, r_send, r_recv, c_send, c_recv, s_send, s_recv,
):
    part, me = lax.axis_index("parts"), lax.axis_index("modes")
    n = lax.axis_size("modes")
    half = n // 2
    quarter = n // 4
    within = me % half
    top = me // half
    second = (me // quarter) % 2
    m_high, m_low, d = within // 4, (within // 2) % 2, within % 2
    inner = top != second
    f32 = jnp.float32
    depth = (n // 2).bit_length()

    def device(index):
        return (part, index)

    def flipped(width):
        return me + width * (1 - 2 * ((me // width) % 2))

    tops = stem.shape[3]
    loads = [pltpu.make_async_copy(w3, raw3, load_sem.at[0])]
    for i in range(tops):
        which = (m_high + tops - 1 - i) % tops
        loads.append(
            pltpu.make_async_copy(stem.at[:, :, :, which], xin.at[i], load_sem.at[1 + i])
        )
    loads.append(pltpu.make_async_copy(b1, raw1, load_sem.at[1 + tops]))
    loads.append(pltpu.make_async_copy(b2, raw2, load_sem.at[2 + tops]))
    for load in loads:
        load.start()
    barrier = pltpu.get_barrier_semaphore()
    for i in range(1, n):
        pl.semaphore_signal(barrier, inc=1, device_id=device((me + i) % n), device_id_type=MESH)

    chunk = raw3.shape[3] // CHUNKS
    loads[0].wait()
    mine = pick[me]
    for k in range(CHUNKS):
        value = raw3[0, :, :, k * chunk : (k + 1) * chunk, :]
        for j in range(1, raw3.shape[0]):
            value = jnp.where(mine == j, raw3[j, :, :, k * chunk : (k + 1) * chunk, :], value)
        own3[k] = value
    pl.semaphore_wait(barrier, n - 1)

    across = (1 - top) * half + (1 - second) * quarter + me % quarter
    opposite = (1 - top) * half + within
    beside = top * half + (1 - second) * quarter + me % quarter

    def to_relay(k):
        return pltpu.make_async_remote_copy(
            own3.at[k], relay3.at[k], r_send.at[k], r_recv.at[k],
            device_id=device(across), device_id_type=MESH,
        )

    def to_cross(k, source, target):
        return pltpu.make_async_remote_copy(
            source.at[k], cross3.at[k], c_send.at[k], c_recv.at[k],
            device_id=device(target), device_id_type=MESH,
        )

    @pl.when(inner)
    def _():
        for k in range(CHUNKS):
            to_relay(k).start()

    entries, lanes = stem.shape[1], stem.shape[5]

    def x_copy(target, source):
        return pltpu.make_async_remote_copy(
            cut.at[target], x.at[:, source], x_send.at[target], x_recv.at[source],
            device_id=device(top * half + target), device_id_type=MESH,
        )

    def piece(z, low, e):
        return (z * 2 + low) * 2 + e

    for i in range(tops):
        loads[1 + i].wait()
        which = (m_high + tops - 1 - i) % tops
        for r in range(2):
            for a in range(2):
                for q in range(lanes // 128):
                    tmp = turned_x.at[(a * 2 + q) % turned_x.shape[0]]
                    tmp[...] = (
                        xin[i, r, :, a, :, q * 128 : (q + 1) * 128]
                        .astype(f32)
                        .reshape(entries * 8, 128)
                    )
                    for row in range(8):
                        low, b, e = row // 4, (row // 2) % 2, row % 2
                        at = (a * 2 + b) * lanes + q * 128
                        cut[piece(which, low, e), r, :, at : at + 128] = tmp[
                            pl.ds(row, entries, stride=8), :
                        ].astype(cut.dtype)
        for low in range(2):
            for e in range(2):
                target = piece(which, (m_low + 1 - low) % 2, (d + 1 - e) % 2)
                if i == tops - 1 and low == 1 and e == 1:
                    x[:, within] = cut[within]
                else:
                    x_copy(target, within).start()

    loads[1 + tops].wait()
    spread(order, 0, top * w1.shape[1] // 2, onehot.at[:, : onehot.shape[1] // 2])
    turn(raw1, onehot.at[:, : onehot.shape[1] // 2], w1)
    loads[2 + tops].wait()
    spread(order, 1, 0, onehot)
    turn(raw2, onehot, w2)

    for step in range(1, half):
        source = (within + step) % half
        x_copy(source, source).wait_recv()
    for step in range(1, half):
        x_copy((within + step) % half, within).wait_send()

    @pl.when(inner)
    def _():
        for k in range(CHUNKS):
            to_relay(k).wait()
            to_cross(k, relay3, beside).start()

    @pl.when(jnp.logical_not(inner))
    def _():
        for k in range(CHUNKS):
            to_cross(k, own3, opposite).start()

    legs = w1.shape[1]
    tile = 256
    columns = x.shape[3] // 2
    tiles = legs // 2 // tile

    @pl.loop(0, tiles)
    def _(i):
        for t in range(2):
            for r in range(2):
                rows = pl.ds(pl.multiple_of(t * (legs // 2) + i * tile, tile), tile)
                y = jnp.dot(
                    w1[r, rows, :], x[...].reshape(legs, 2 * columns), preferred_element_type=f32
                ).astype(mid.dtype)
                for a in range(2):
                    to = pl.ds(pl.multiple_of((r * 2 + a) * (legs // 2) + i * tile, tile), tile)
                    mid[to, t * columns : (t + 1) * columns] = y[
                        :, a * columns : (a + 1) * columns
                    ]

    @pl.loop(0, tiles)
    def _(i):
        for u in range(2):
            for r in range(2):
                rows = pl.ds(pl.multiple_of(u * (legs // 2) + i * tile, tile), tile)
                y = jnp.dot(w2[r, rows, :], mid[...], preferred_element_type=f32).astype(y2.dtype)
                to = pl.ds(pl.multiple_of(i * tile, tile), tile)
                for t in range(2):
                    y2[(t + top) % 2, r, to, u * columns : (u + 1) * columns] = y[
                        :, t * columns : (t + 1) * columns
                    ]

    def applied(w, t):
        return jnp.dot(
            blocks(w), y2[t].reshape(legs, 2 * columns), preferred_element_type=f32
        )

    @pl.loop(0, CHUNKS)
    def _(k):
        acc[k] = applied(own3.at[k], 0)

    def exchange(stage, k):
        return pltpu.make_async_remote_copy(
            sends[stage].at[k], gots[stage].at[k], s_send.at[stage, k], s_recv.at[stage, k],
            device_id=device(flipped(1 << stage)), device_id_type=MESH,
        )

    def split(stage, k, total):
        bit = (me // (1 << stage)) % 2
        pairs = total.reshape(2, total.shape[1] // 2, 2, chunk, 2 * columns)
        keeps[stage][k] = jnp.where(bit == 0, pairs[:, :, 0], pairs[:, :, 1])
        sends[stage][k] = jnp.where(bit == 0, pairs[:, :, 1], pairs[:, :, 0]).astype(
            sends[stage].dtype
        )
        exchange(stage, k).start()

    def joined(stage, k):
        exchange(stage, k).wait_recv()
        return keeps[stage][k] + gots[stage][k].astype(f32)

    for step in range(CHUNKS + depth):
        for stage in range(depth, 0, -1):
            k = step - stage
            if 0 <= k < CHUNKS:
                total = joined(stage - 1, k)
                if stage < depth:
                    split(stage, k, total)
                else:
                    out[:, k * chunk : (k + 1) * chunk, :] = total[:, 0].astype(out.dtype)
        if step < CHUNKS:
            to_cross(step, own3, opposite).wait_recv()
            total = acc[step] + applied(cross3.at[step], 1)
            split(0, step, total.reshape(2, n, chunk, 2 * columns))

    @pl.when(inner)
    def _():
        for k in range(CHUNKS):
            to_cross(k, relay3, beside).wait_send()

    @pl.when(jnp.logical_not(inner))
    def _():
        for k in range(CHUNKS):
            to_cross(k, own3, opposite).wait_send()

    for stage in range(depth):
        for k in range(CHUNKS):
            exchange(stage, k).wait_send()


def by_halves(stem, branch_one, branch_two, branch_three, leg_orders, slice_pick):
    n = lax.axis_size("modes")
    entries, heads, lanes = stem.shape[2], stem.shape[3], stem.shape[4]
    slices, out_width, depth3 = branch_three.shape[0], branch_three.shape[3], branch_three.shape[4]
    legs = branch_one.shape[1]
    mine, tops = out_width // n, n // 8
    chunk = mine // CHUNKS
    stages = (n // 2).bit_length()
    cut = stem.reshape(2, entries, 2, tops, 8, lanes)
    third = branch_three.reshape(slices, 2, n, mine, depth3)
    bf16, f32 = jnp.bfloat16, jnp.float32
    smem = pl.BlockSpec(memory_space=pltpu.SMEM)
    anyspace = pl.BlockSpec(memory_space=pl.ANY)
    dma = pltpu.SemaphoreType.DMA

    def halving(dtype):
        return [
            pltpu.VMEM((CHUNKS, 2, n >> (s + 1), chunk, 4 * lanes), dtype) for s in range(stages)
        ]

    out = pl.pallas_call(
        contraction,
        name="contraction",
        out_shape=jax.ShapeDtypeStruct((2, mine, 4 * lanes), bf16),
        in_specs=[smem, smem] + [anyspace] * 4,
        out_specs=pl.BlockSpec(memory_space=pltpu.VMEM),
        scratch_shapes=[
            pltpu.VMEM((tops, 2, entries, 2, 8, lanes), bf16),
            pltpu.VMEM((4, entries * 8, 128), f32),
            pltpu.VMEM((n // 2, 2, entries, 4 * lanes), bf16),
            pltpu.VMEM((2, n // 2, entries, 4 * lanes), bf16),
            pltpu.VMEM(branch_one.shape, bf16),
            pltpu.VMEM(branch_two.shape, bf16),
            pltpu.VMEM((legs, legs), bf16),
            pltpu.VMEM((2, legs, legs), bf16),
            pltpu.VMEM((2, legs, 2 * legs), bf16),
            pltpu.VMEM((2 * legs, 4 * lanes), bf16),
            pltpu.VMEM((2, 2, legs // 2, 4 * lanes), bf16),
            pltpu.VMEM(third.shape, bf16),
            pltpu.VMEM((CHUNKS, 2, n, chunk, depth3), bf16),
            pltpu.VMEM((CHUNKS, 2, n, chunk, depth3), bf16),
            pltpu.VMEM((CHUNKS, 2, n, chunk, depth3), bf16),
            pltpu.VMEM((CHUNKS, 2 * n * chunk, 4 * lanes), f32),
            halving(f32),
            halving(bf16),
            halving(bf16),
            dma((3 + tops,)),
            dma((n // 2,)),
            dma((n // 2,)),
            dma((CHUNKS,)),
            dma((CHUNKS,)),
            dma((CHUNKS,)),
            dma((CHUNKS,)),
            dma((stages, CHUNKS)),
            dma((stages, CHUNKS)),
        ],
        compiler_params=pltpu.CompilerParams(
            collective_id=0, has_side_effects=True, vmem_limit_bytes=62 * 2**20
        ),
    )(leg_orders, slice_pick, cut, branch_one, branch_two, third)
    return out.reshape(2, mine, 2, 2, lanes).transpose(1, 0, 2, 3, 4)


def per_device(stem, branch_one, branch_two, branch_three, leg_orders, slice_pick):
    groups = lax.axis_size("modes")
    whole_tiles = (
        groups & (groups - 1) == 0
        and stem.shape[2] % 16 == 0
        and branch_three.shape[3] % (groups * CHUNKS * 8) == 0
    )
    program = by_halves if whole_tiles else by_columns
    return program(stem, branch_one, branch_two, branch_three, leg_orders, slice_pick)


def solution(mesh):
    in_specs = (
        P(None, "modes", None, None, "parts"),
        P(),
        P(),
        P(None, None, "modes", None, None),
        P(),
        P("parts"),
    )
    out_specs = P(("parts", "modes"), None, None, None, None)
    return jax.shard_map(
        per_device, mesh=mesh, in_specs=in_specs, out_specs=out_specs, check_vma=False
    )
```

```python
import jax
import jax.numpy as jnp
from jax import lax
from jax.experimental import pallas as pl
from jax.experimental.pallas import tpu as pltpu
from jax.sharding import PartitionSpec as P

TILES = 4
CHUNKS = 4
MESH = pl.DeviceIdType.MESH


def turn_columns(order, branch, out, onehot):
    width = branch.shape[1]

    @pl.when(pl.program_id(0) == 0)
    def _():
        positions = lax.broadcasted_iota(jnp.int32, (1, width), 1)
        source = jnp.zeros((1, width), jnp.int32)
        for bit in range(order.shape[0]):
            source += jnp.left_shift(jnp.right_shift(positions, bit) & 1, order[bit])
        rows = lax.broadcasted_iota(jnp.int32, (width, width), 0)
        onehot[...] = jnp.where(rows == source, 1.0, 0.0).astype(onehot.dtype)

    out[...] = jnp.dot(
        branch[...], onehot[...], preferred_element_type=jnp.float32
    ).astype(out.dtype)


def turned(branch, order, name):
    width = branch.shape[2]
    flat = branch.reshape(-1, width)
    tile = flat.shape[0] // 8
    out = pl.pallas_call(
        turn_columns,
        name=name,
        grid=(8,),
        out_shape=jax.ShapeDtypeStruct(flat.shape, flat.dtype),
        in_specs=[
            pl.BlockSpec(memory_space=pltpu.SMEM),
            pl.BlockSpec((tile, width), lambda i: (i, 0)),
        ],
        out_specs=pl.BlockSpec((tile, width), lambda i: (i, 0)),
        scratch_shapes=[pltpu.VMEM((width, width), flat.dtype)],
        compiler_params=pltpu.CompilerParams(vmem_limit_bytes=58 * 2**20),
        cost_estimate=pl.CostEstimate(
            flops=2 * flat.shape[0] * width * width,
            bytes_accessed=4 * flat.size,
            transcendentals=0,
        ),
    )(order, flat)
    return out.reshape(branch.shape)


def complex_tile(w, values):
    half = values.shape[1] // 2
    p = jnp.dot(w[0], values, preferred_element_type=jnp.float32)
    q = jnp.dot(w[1], values, preferred_element_type=jnp.float32)
    real = p[:, :half] - q[:, half:]
    imag = p[:, half:] + q[:, :half]
    return real.astype(jnp.bfloat16), imag.astype(jnp.bfloat16)


def two_branches(x_hbm, w1_hbm, w2_hbm, out, x, w1, w2, mid, sems):
    width = x.shape[0]
    half = width // 2
    tile = width // TILES
    lanes = x.shape[1] // 8
    copies = [pltpu.make_async_copy(x_hbm, x, sems.at[0])]
    for which, (source, target) in enumerate(((w1_hbm, w1), (w2_hbm, w2))):
        for i in range(TILES):
            rows = pl.ds(i * tile, tile)
            copies.append(
                pltpu.make_async_copy(
                    source.at[:, rows, :], target.at[:, rows, :], sems.at[1 + which * TILES + i]
                )
            )
    for copy in copies:
        copy.start()
    copies[0].wait()
    for i in range(TILES):
        copies[1 + i].wait()
        t, c = divmod(i * tile, half)
        parts = complex_tile(w1[:, i * tile : (i + 1) * tile, :], x[...])
        for r in range(2):
            for a in range(2):
                at = (2 * r + t) * 2 * lanes
                mid[a * half + c : a * half + c + tile, at : at + 2 * lanes] = parts[r][
                    :, a * 2 * lanes : (a + 1) * 2 * lanes
                ]
    for i in range(TILES):
        copies[1 + TILES + i].wait()
        u, c = divmod(i * tile, half)
        parts = complex_tile(w2[:, i * tile : (i + 1) * tile, :], mid[...])
        for r in range(2):
            for td in range(4):
                at = (2 * r + u) * lanes
                out[td, c : c + tile, at : at + lanes] = parts[r][:, td * lanes : (td + 1) * lanes]


def third_branch(place, wa, wb, wc, wd, values, out):
    k2 = place[0]
    k0 = place[1]
    half = values.shape[2] // 2
    p = q = None
    for w, t, d in ((wa, k2, k0), (wb, 1 - k2, k0), (wc, k2, 1 - k0), (wd, 1 - k2, 1 - k0)):
        block = values[2 * t + d]
        pp = jnp.dot(w[0], block, preferred_element_type=jnp.float32)
        qq = jnp.dot(w[1], block, preferred_element_type=jnp.float32)
        p = pp if p is None else p + pp
        q = qq if q is None else q + qq
    out[:, :half] = (p[:, :half] - q[:, half:]).astype(out.dtype)
    out[:, half:] = (p[:, half:] + q[:, :half]).astype(out.dtype)


def by_columns(stem, branch_one, branch_two, branch_three, leg_orders, slice_pick):
    groups = lax.axis_size("modes")
    me = lax.axis_index("modes")
    rest = groups // 8
    entries, lanes = stem.shape[2], stem.shape[4] // 2
    k2 = (me // (2 * rest)) % 2
    quarter = me // (2 * rest)
    k0 = me % 2

    cut = stem.reshape(2, entries, 2, 2, rest, 2, 2, 2, lanes)
    cut = cut.transpose(3, 7, 4, 5, 1, 0, 2, 6, 8).reshape(groups, entries, 8 * lanes)
    pick = lax.dynamic_index_in_dim(slice_pick, me, 0, keepdims=False)
    own = lax.dynamic_index_in_dim(branch_three, pick, 0, keepdims=False)[:, 0]
    q = 2 * rest
    middle = [(q + i, 2 * q + i) for i in range(q)]
    middle += [(b, a) for a, b in middle]
    outer = [(i, i ^ q) for i in range(groups)] if q & (q - 1) == 0 else [
        (i, i + q if (i // q) % 2 == 0 else i - q) for i in range(groups)
    ]
    cores = [(i, i ^ 1) for i in range(groups)]
    crossed = lax.ppermute(own, "modes", middle)
    w1 = turned(branch_one, leg_orders[0], "turn_one")
    cut, crossed, w1, branch_two = lax.optimization_barrier((cut, crossed, w1, branch_two))
    arrived = lax.all_to_all(cut, "modes", split_axis=0, concat_axis=0, tiled=True)
    x = arrived.reshape(groups * entries, 8 * lanes)
    w2 = turned(branch_two, leg_orders[1], "turn_two")
    crossed, w2 = lax.optimization_barrier((crossed, w2))
    inner = (quarter == 1) | (quarter == 2)
    wa = jnp.where(inner, crossed, own)
    wb = lax.ppermute(wa, "modes", outer)
    wc = lax.ppermute(wa, "modes", cores)
    wd = lax.ppermute(wb, "modes", cores)

    width = w1.shape[1]
    half = width // 2
    any_spec = pl.BlockSpec(memory_space=pl.ANY)
    vmem = pl.BlockSpec(memory_space=pltpu.VMEM)
    values = pl.pallas_call(
        two_branches,
        name="two_branches",
        out_shape=jax.ShapeDtypeStruct((4, half, 4 * lanes), jnp.bfloat16),
        in_specs=[any_spec] * 3,
        out_specs=vmem,
        scratch_shapes=[
            pltpu.VMEM(x.shape, x.dtype),
            pltpu.VMEM(w1.shape, w1.dtype),
            pltpu.VMEM(w2.shape, w2.dtype),
            pltpu.VMEM((width, 8 * lanes), jnp.bfloat16),
            pltpu.SemaphoreType.DMA((1 + 2 * TILES,)),
        ],
        compiler_params=pltpu.CompilerParams(vmem_limit_bytes=58 * 2**20),
        cost_estimate=pl.CostEstimate(
            flops=8 * width * width * 8 * lanes, bytes_accessed=12 * 2**20, transcendentals=0
        ),
    )(x, w1, w2)

    out_width = own.shape[1]
    partial = pl.pallas_call(
        third_branch,
        name="third_branch",
        out_shape=jax.ShapeDtypeStruct((out_width, 4 * lanes), jnp.bfloat16),
        in_specs=[pl.BlockSpec(memory_space=pltpu.SMEM)] + [vmem] * 5,
        out_specs=vmem,
        compiler_params=pltpu.CompilerParams(vmem_limit_bytes=24 * 2**20),
        cost_estimate=pl.CostEstimate(
            flops=16 * out_width * half * 4 * lanes, bytes_accessed=7 * 2**20, transcendentals=0
        ),
    )(jnp.stack([k2, k0]).astype(jnp.int32), wa, wb, wc, wd, values)

    pieces = lax.all_to_all(partial, "modes", split_axis=0, concat_axis=0, tiled=True)
    mine = out_width // groups
    pieces = pieces.reshape(2, 2, rest, 2, mine, 2, 2, lanes).astype(jnp.float32)
    summed = jnp.sum(pieces, axis=(0, 2)).astype(jnp.bfloat16)
    return summed.transpose(2, 3, 4, 1, 0, 5).reshape(mine, 2, 2, 2, 2 * lanes)


def spread(order, which, start, onehot):
    rows, width = onehot.shape
    positions = start + lax.broadcasted_iota(jnp.int32, (1, width), 1)
    source = jnp.zeros((1, width), jnp.int32)
    for bit in range(order.shape[1]):
        source += jnp.left_shift(jnp.right_shift(positions, bit) & 1, order[which, bit])
    tile = 256

    @pl.loop(0, rows // tile)
    def _(i):
        at = i * tile + lax.broadcasted_iota(jnp.int32, (tile, width), 0)
        onehot[pl.ds(pl.multiple_of(i * tile, tile), tile), :] = jnp.where(
            at == source, 1.0, 0.0
        ).astype(onehot.dtype)


def turn_first(branch, onehot, w1):
    rows, tile = branch.shape[1], 256
    for t in range(2):

        @pl.loop(0, rows // 2 // tile)
        def _(i):
            to = pl.ds(pl.multiple_of(i * tile, tile), tile)
            at = pl.ds(pl.multiple_of(t * (rows // 2) + i * tile, tile), tile)
            for r in range(2):
                w1[t, r, to, :] = jnp.dot(
                    branch[r, at, :], onehot[...], preferred_element_type=jnp.float32
                ).astype(w1.dtype)


def turn_second(branch, onehot, w2):
    rows, tile = branch.shape[1], 256
    half = rows // 2

    @pl.loop(0, rows // tile)
    def _(i):
        at = pl.ds(pl.multiple_of(i * tile, tile), tile)
        real = jnp.dot(branch[0, at, :], onehot[...], preferred_element_type=jnp.float32)
        real = real.astype(w2.dtype)
        for a in range(2):
            w2[0, a, at, :half] = real[:, a * half : (a + 1) * half]
            w2[1, a, at, half:] = real[:, a * half : (a + 1) * half]
        imag = jnp.dot(branch[1, at, :], onehot[...], preferred_element_type=jnp.float32)
        imag = imag.astype(w2.dtype)
        for a in range(2):
            w2[0, a, at, half:] = -imag[:, a * half : (a + 1) * half]
            w2[1, a, at, :half] = imag[:, a * half : (a + 1) * half]


def joined_branches(w1, w2, w21):
    rows, tile = w2.shape[2], 256
    legs = w1.shape[3]

    @pl.loop(0, rows // tile)
    def _(i):
        at = pl.ds(pl.multiple_of(i * tile, tile), tile)
        for t in range(2):
            first = w1[t].reshape(2 * w1.shape[2], legs)
            for a in range(2):
                lo, hi = a * legs, (2 + a) * legs
                real = jnp.dot(w2[0, a, at, :], first, preferred_element_type=jnp.float32)
                real = real.astype(w21.dtype)
                w21[t, 0, at, lo : lo + legs] = real
                w21[t, 1, at, hi : hi + legs] = real
                imag = jnp.dot(w2[1, a, at, :], first, preferred_element_type=jnp.float32)
                imag = imag.astype(w21.dtype)
                w21[t, 0, at, hi : hi + legs] = -imag
                w21[t, 1, at, lo : lo + legs] = imag


def blocks(w):
    rows = w.shape[1] * w.shape[2]
    real = w[0].astype(jnp.float32).reshape(rows, w.shape[3])
    imag = w[1].astype(jnp.float32).reshape(rows, w.shape[3])
    return jnp.concatenate(
        [jnp.concatenate([real, -imag], axis=1), jnp.concatenate([imag, real], axis=1)], axis=0
    ).astype(w.dtype)


def contraction(
    order, pick, stem, b1, b2, w3, out,
    xin, turned_x, cut, x, raw1, raw2, onehot, w1, w2, w21, y2, raw3, own3, relay3, cross3, acc,
    keeps, sends, gots, load_sem, x_send, x_recv, r_send, r_recv, c_send, c_recv, s_send, s_recv,
):
    part, me = lax.axis_index("parts"), lax.axis_index("modes")
    n = lax.axis_size("modes")
    half = n // 2
    quarter = n // 4
    within = me % half
    top = me // half
    second = (me // quarter) % 2
    m_high, m_low, d = within // 4, (within // 2) % 2, within % 2
    inner = top != second
    f32 = jnp.float32
    depth = (n // 2).bit_length()

    def device(index):
        return (part, index)

    def flipped(width):
        return me + width * (1 - 2 * ((me // width) % 2))

    tops = stem.shape[3]
    loads = [pltpu.make_async_copy(w3, raw3, load_sem.at[0])]
    for i in range(tops):
        which = (m_high + tops - 1 - i) % tops
        loads.append(
            pltpu.make_async_copy(stem.at[:, :, :, which], xin.at[i], load_sem.at[1 + i])
        )
    loads.append(pltpu.make_async_copy(b1, raw1, load_sem.at[1 + tops]))
    loads.append(pltpu.make_async_copy(b2, raw2, load_sem.at[2 + tops]))
    for load in loads:
        load.start()
    barrier = pltpu.get_barrier_semaphore()
    across = (1 - top) * half + (1 - second) * quarter + me % quarter
    opposite = (1 - top) * half + within
    beside = top * half + (1 - second) * quarter + me % quarter
    peers = [top * half + (within + i) % half for i in range(1, half)] + [across, opposite]
    for peer in peers:
        pl.semaphore_signal(barrier, inc=1, device_id=device(peer), device_id_type=MESH)

    chunk = raw3.shape[3] // CHUNKS
    loads[0].wait()
    mine = pick[me]
    for k in range(CHUNKS):
        value = raw3[0, :, :, k * chunk : (k + 1) * chunk, :]
        for j in range(1, raw3.shape[0]):
            value = jnp.where(mine == j, raw3[j, :, :, k * chunk : (k + 1) * chunk, :], value)
        own3[k] = value

    def to_relay(k):
        return pltpu.make_async_remote_copy(
            own3.at[k], relay3.at[k], r_send.at[k], r_recv.at[k],
            device_id=device(across), device_id_type=MESH,
        )

    def to_cross(k, source, target):
        return pltpu.make_async_remote_copy(
            source.at[k], cross3.at[k], c_send.at[k], c_recv.at[k],
            device_id=device(target), device_id_type=MESH,
        )

    entries, lanes = stem.shape[1], stem.shape[5]

    def x_copy(target, source):
        return pltpu.make_async_remote_copy(
            cut.at[target], x.at[:, :, source], x_send.at[target], x_recv.at[source],
            device_id=device(top * half + target), device_id_type=MESH,
        )

    def piece(z, low, e):
        return (z * 2 + low) * 2 + e

    for i in range(tops):
        loads[1 + i].wait()
        which = (m_high + tops - 1 - i) % tops
        for r in range(2):
            for a in range(2):
                for q in range(lanes // 128):
                    tmp = turned_x.at[(a * 2 + q) % turned_x.shape[0]]
                    tmp[...] = (
                        xin[i, r, :, a, :, q * 128 : (q + 1) * 128]
                        .astype(f32)
                        .reshape(entries * 8, 128)
                    )
                    for row in range(8):
                        low, b, e = row // 4, (row // 2) % 2, row % 2
                        at = b * lanes + q * 128
                        cut[piece(which, low, e), r, a, :, at : at + 128] = tmp[
                            pl.ds(row, entries, stride=8), :
                        ].astype(cut.dtype)
    pl.semaphore_wait(barrier, len(peers))

    @pl.when(inner)
    def _():
        for k in range(CHUNKS):
            to_relay(k).start()

    for i in range(tops):
        which = (m_high + tops - 1 - i) % tops
        for low in range(2):
            for e in range(2):
                if i < tops - 1 or low == 0 or e == 0:
                    target = piece(which, (m_low + 1 - low) % 2, (d + 1 - e) % 2)
                    x_copy(target, within).start()
    x[:, :, within] = cut[within]

    loads[1 + tops].wait()
    legs = w1.shape[3]
    spread(order, 0, top * legs, onehot.at[:, :legs])
    turn_first(raw1, onehot.at[:, :legs], w1)
    loads[2 + tops].wait()
    spread(order, 1, 0, onehot)
    turn_second(raw2, onehot, w2)
    joined_branches(w1, w2, w21)

    for step in range(1, half):
        x_copy((within + step) % half, within).wait_send()

    @pl.when(inner)
    def _():
        for k in range(CHUNKS):
            to_relay(k).wait()
            to_cross(k, relay3, beside).start()

    @pl.when(jnp.logical_not(inner))
    def _():
        for k in range(CHUNKS):
            to_cross(k, own3, opposite).start()

    for step in range(1, half):
        source = (within + step) % half
        x_copy(source, source).wait_recv()

    tile, columns = 256, x.shape[4]

    @pl.loop(0, legs // tile)
    def _(i):
        values = x[...].reshape(4 * legs, columns)
        for u in range(2):
            rows = pl.ds(pl.multiple_of(u * legs + i * tile, tile), tile)
            to = pl.ds(pl.multiple_of(i * tile, tile), tile)
            for t in range(2):
                for r in range(2):
                    y2[(t + top) % 2, r, to, u * columns : (u + 1) * columns] = jnp.dot(
                        w21[t, r, rows, :], values, preferred_element_type=f32
                    ).astype(y2.dtype)

    def applied(w, t):
        return jnp.dot(
            blocks(w), y2[t].reshape(2 * legs, 2 * columns), preferred_element_type=f32
        )

    widths = [1 << s for s in range(depth)]
    orders = [widths, widths[:1] + widths[1:-1][::-1] + widths[-1:]]

    def exchange(u, stage, k):
        return pltpu.make_async_remote_copy(
            sends[stage].at[u, k], gots[stage].at[u, k],
            s_send.at[u, stage, k], s_recv.at[u, stage, k],
            device_id=device(flipped(orders[u][stage])), device_id_type=MESH,
        )

    def split(u, stage, k, total):
        width = orders[u][stage]
        left = sorted(orders[u][stage:], reverse=True)
        axis = 1 + left.index(width)
        pairs = total.reshape((2,) + (2,) * len(left) + (chunk, columns))
        pick_of = (slice(None),) * axis
        zero, one = pairs[pick_of + (0,)], pairs[pick_of + (1,)]
        bit = (me // width) % 2
        shape = keeps[stage].shape[2:]
        keeps[stage][u, k] = jnp.where(bit == 0, zero, one).reshape(shape)
        sends[stage][u, k] = jnp.where(bit == 0, one, zero).reshape(shape).astype(
            sends[stage].dtype
        )
        exchange(u, stage, k).start()

    def advance(stage, k):
        for u in range(2):
            exchange(u, stage - 1, k).wait_recv()
            total = keeps[stage - 1][u, k] + gots[stage - 1][u, k].astype(f32)
            if stage < depth:
                split(u, stage, k, total)
            else:
                out[:, k * chunk : (k + 1) * chunk, u * columns : (u + 1) * columns] = total[
                    :, 0
                ].astype(out.dtype)

    for step in range(CHUNKS + depth):
        if step < CHUNKS:
            acc[...] = applied(own3.at[step], 0)
            to_cross(step, own3, opposite).wait_recv()
            total = acc[...] + applied(cross3.at[step], 1)
            for u in range(2):
                part_of = total[:, u * columns : (u + 1) * columns]
                split(u, 0, step, part_of.reshape(2, n, chunk, columns))
        for stage in range(depth, 0, -1):
            k = step - stage + 1
            if 0 <= k < CHUNKS:
                advance(stage, k)

    @pl.when(inner)
    def _():
        for k in range(CHUNKS):
            to_cross(k, relay3, beside).wait_send()

    @pl.when(jnp.logical_not(inner))
    def _():
        for k in range(CHUNKS):
            to_cross(k, own3, opposite).wait_send()

    for stage in range(depth):
        for k in range(CHUNKS):
            for u in range(2):
                exchange(u, stage, k).wait_send()


def by_halves(stem, branch_one, branch_two, branch_three, leg_orders, slice_pick):
    n = lax.axis_size("modes")
    entries, heads, lanes = stem.shape[2], stem.shape[3], stem.shape[4]
    slices, out_width, depth3 = branch_three.shape[0], branch_three.shape[3], branch_three.shape[4]
    legs = branch_one.shape[1]
    mine, tops = out_width // n, n // 8
    chunk = mine // CHUNKS
    stages = (n // 2).bit_length()
    cut = stem.reshape(2, entries, 2, tops, 8, lanes)
    third = branch_three.reshape(slices, 2, n, mine, depth3)
    bf16, f32 = jnp.bfloat16, jnp.float32
    smem = pl.BlockSpec(memory_space=pltpu.SMEM)
    anyspace = pl.BlockSpec(memory_space=pl.ANY)
    dma = pltpu.SemaphoreType.DMA

    def halving(dtype):
        return [
            pltpu.VMEM((2, CHUNKS, 2, n >> (s + 1), chunk, 2 * lanes), dtype)
            for s in range(stages)
        ]

    out = pl.pallas_call(
        contraction,
        name="contraction",
        out_shape=jax.ShapeDtypeStruct((2, mine, 4 * lanes), bf16),
        in_specs=[smem, smem] + [anyspace] * 4,
        out_specs=pl.BlockSpec(memory_space=pltpu.VMEM),
        scratch_shapes=[
            pltpu.VMEM((tops, 2, entries, 2, 8, lanes), bf16),
            pltpu.VMEM((4, entries * 8, 128), f32),
            pltpu.VMEM((n // 2, 2, 2, entries, 2 * lanes), bf16),
            pltpu.VMEM((2, 2, n // 2, entries, 2 * lanes), bf16),
            pltpu.VMEM(branch_one.shape, bf16),
            pltpu.VMEM(branch_two.shape, bf16),
            pltpu.VMEM((legs, legs), bf16),
            pltpu.VMEM((2, 2, legs // 2, legs // 2), bf16),
            pltpu.VMEM((2, 2, legs, legs), bf16),
            pltpu.VMEM((2, 2, legs, 2 * legs), bf16),
            pltpu.VMEM((2, 2, legs // 2, 4 * lanes), bf16),
            pltpu.VMEM(third.shape, bf16),
            pltpu.VMEM((CHUNKS, 2, n, chunk, depth3), bf16),
            pltpu.VMEM((CHUNKS, 2, n, chunk, depth3), bf16),
            pltpu.VMEM((CHUNKS, 2, n, chunk, depth3), bf16),
            pltpu.VMEM((2 * n * chunk, 4 * lanes), f32),
            halving(f32),
            halving(bf16),
            halving(bf16),
            dma((3 + tops,)),
            dma((n // 2,)),
            dma((n // 2,)),
            dma((CHUNKS,)),
            dma((CHUNKS,)),
            dma((CHUNKS,)),
            dma((CHUNKS,)),
            dma((2, stages, CHUNKS)),
            dma((2, stages, CHUNKS)),
        ],
        compiler_params=pltpu.CompilerParams(
            collective_id=0, has_side_effects=True, vmem_limit_bytes=62 * 2**20
        ),
    )(leg_orders, slice_pick, cut, branch_one, branch_two, third)
    return out.reshape(2, mine, 2, 2, lanes).transpose(1, 0, 2, 3, 4)


def per_device(stem, branch_one, branch_two, branch_three, leg_orders, slice_pick):
    groups = lax.axis_size("modes")
    whole_tiles = (
        groups & (groups - 1) == 0
        and stem.shape[2] % 16 == 0
        and branch_three.shape[3] % (groups * CHUNKS * 8) == 0
    )
    program = by_halves if whole_tiles else by_columns
    return program(stem, branch_one, branch_two, branch_three, leg_orders, slice_pick)


def solution(mesh):
    in_specs = (
        P(None, "modes", None, None, "parts"),
        P(),
        P(),
        P(None, None, "modes", None, None),
        P(),
        P("parts"),
    )
    out_specs = P(("parts", "modes"), None, None, None, None)
    return jax.shard_map(
        per_device, mesh=mesh, in_specs=in_specs, out_specs=out_specs, check_vma=False
    )
```

```python
import jax
import jax.numpy as jnp
from jax import lax
from jax.experimental import pallas as pl
from jax.experimental.pallas import tpu as pltpu
from jax.sharding import PartitionSpec as P

TILES = 4
CHUNKS = 4
MESH = pl.DeviceIdType.MESH


def turn_columns(order, branch, out, onehot):
    width = branch.shape[1]

    @pl.when(pl.program_id(0) == 0)
    def _():
        positions = lax.broadcasted_iota(jnp.int32, (1, width), 1)
        source = jnp.zeros((1, width), jnp.int32)
        for bit in range(order.shape[0]):
            source += jnp.left_shift(jnp.right_shift(positions, bit) & 1, order[bit])
        rows = lax.broadcasted_iota(jnp.int32, (width, width), 0)
        onehot[...] = jnp.where(rows == source, 1.0, 0.0).astype(onehot.dtype)

    out[...] = jnp.dot(
        branch[...], onehot[...], preferred_element_type=jnp.float32
    ).astype(out.dtype)


def turned(branch, order, name):
    width = branch.shape[2]
    flat = branch.reshape(-1, width)
    tile = flat.shape[0] // 8
    out = pl.pallas_call(
        turn_columns,
        name=name,
        grid=(8,),
        out_shape=jax.ShapeDtypeStruct(flat.shape, flat.dtype),
        in_specs=[
            pl.BlockSpec(memory_space=pltpu.SMEM),
            pl.BlockSpec((tile, width), lambda i: (i, 0)),
        ],
        out_specs=pl.BlockSpec((tile, width), lambda i: (i, 0)),
        scratch_shapes=[pltpu.VMEM((width, width), flat.dtype)],
        compiler_params=pltpu.CompilerParams(vmem_limit_bytes=58 * 2**20),
        cost_estimate=pl.CostEstimate(
            flops=2 * flat.shape[0] * width * width,
            bytes_accessed=4 * flat.size,
            transcendentals=0,
        ),
    )(order, flat)
    return out.reshape(branch.shape)


def complex_tile(w, values):
    half = values.shape[1] // 2
    p = jnp.dot(w[0], values, preferred_element_type=jnp.float32)
    q = jnp.dot(w[1], values, preferred_element_type=jnp.float32)
    real = p[:, :half] - q[:, half:]
    imag = p[:, half:] + q[:, :half]
    return real.astype(jnp.bfloat16), imag.astype(jnp.bfloat16)


def two_branches(x_hbm, w1_hbm, w2_hbm, out, x, w1, w2, mid, sems):
    width = x.shape[0]
    half = width // 2
    tile = width // TILES
    lanes = x.shape[1] // 8
    copies = [pltpu.make_async_copy(x_hbm, x, sems.at[0])]
    for which, (source, target) in enumerate(((w1_hbm, w1), (w2_hbm, w2))):
        for i in range(TILES):
            rows = pl.ds(i * tile, tile)
            copies.append(
                pltpu.make_async_copy(
                    source.at[:, rows, :], target.at[:, rows, :], sems.at[1 + which * TILES + i]
                )
            )
    for copy in copies:
        copy.start()
    copies[0].wait()
    for i in range(TILES):
        copies[1 + i].wait()
        t, c = divmod(i * tile, half)
        parts = complex_tile(w1[:, i * tile : (i + 1) * tile, :], x[...])
        for r in range(2):
            for a in range(2):
                at = (2 * r + t) * 2 * lanes
                mid[a * half + c : a * half + c + tile, at : at + 2 * lanes] = parts[r][
                    :, a * 2 * lanes : (a + 1) * 2 * lanes
                ]
    for i in range(TILES):
        copies[1 + TILES + i].wait()
        u, c = divmod(i * tile, half)
        parts = complex_tile(w2[:, i * tile : (i + 1) * tile, :], mid[...])
        for r in range(2):
            for td in range(4):
                at = (2 * r + u) * lanes
                out[td, c : c + tile, at : at + lanes] = parts[r][:, td * lanes : (td + 1) * lanes]


def third_branch(place, wa, wb, wc, wd, values, out):
    k2 = place[0]
    k0 = place[1]
    half = values.shape[2] // 2
    p = q = None
    for w, t, d in ((wa, k2, k0), (wb, 1 - k2, k0), (wc, k2, 1 - k0), (wd, 1 - k2, 1 - k0)):
        block = values[2 * t + d]
        pp = jnp.dot(w[0], block, preferred_element_type=jnp.float32)
        qq = jnp.dot(w[1], block, preferred_element_type=jnp.float32)
        p = pp if p is None else p + pp
        q = qq if q is None else q + qq
    out[:, :half] = (p[:, :half] - q[:, half:]).astype(out.dtype)
    out[:, half:] = (p[:, half:] + q[:, :half]).astype(out.dtype)


def by_columns(stem, branch_one, branch_two, branch_three, leg_orders, slice_pick):
    groups = lax.axis_size("modes")
    me = lax.axis_index("modes")
    rest = groups // 8
    entries, lanes = stem.shape[2], stem.shape[4] // 2
    k2 = (me // (2 * rest)) % 2
    quarter = me // (2 * rest)
    k0 = me % 2

    cut = stem.reshape(2, entries, 2, 2, rest, 2, 2, 2, lanes)
    cut = cut.transpose(3, 7, 4, 5, 1, 0, 2, 6, 8).reshape(groups, entries, 8 * lanes)
    pick = lax.dynamic_index_in_dim(slice_pick, me, 0, keepdims=False)
    own = lax.dynamic_index_in_dim(branch_three, pick, 0, keepdims=False)[:, 0]
    q = 2 * rest
    middle = [(q + i, 2 * q + i) for i in range(q)]
    middle += [(b, a) for a, b in middle]
    outer = [(i, i ^ q) for i in range(groups)] if q & (q - 1) == 0 else [
        (i, i + q if (i // q) % 2 == 0 else i - q) for i in range(groups)
    ]
    cores = [(i, i ^ 1) for i in range(groups)]
    crossed = lax.ppermute(own, "modes", middle)
    w1 = turned(branch_one, leg_orders[0], "turn_one")
    cut, crossed, w1, branch_two = lax.optimization_barrier((cut, crossed, w1, branch_two))
    arrived = lax.all_to_all(cut, "modes", split_axis=0, concat_axis=0, tiled=True)
    x = arrived.reshape(groups * entries, 8 * lanes)
    w2 = turned(branch_two, leg_orders[1], "turn_two")
    crossed, w2 = lax.optimization_barrier((crossed, w2))
    inner = (quarter == 1) | (quarter == 2)
    wa = jnp.where(inner, crossed, own)
    wb = lax.ppermute(wa, "modes", outer)
    wc = lax.ppermute(wa, "modes", cores)
    wd = lax.ppermute(wb, "modes", cores)

    width = w1.shape[1]
    half = width // 2
    any_spec = pl.BlockSpec(memory_space=pl.ANY)
    vmem = pl.BlockSpec(memory_space=pltpu.VMEM)
    values = pl.pallas_call(
        two_branches,
        name="two_branches",
        out_shape=jax.ShapeDtypeStruct((4, half, 4 * lanes), jnp.bfloat16),
        in_specs=[any_spec] * 3,
        out_specs=vmem,
        scratch_shapes=[
            pltpu.VMEM(x.shape, x.dtype),
            pltpu.VMEM(w1.shape, w1.dtype),
            pltpu.VMEM(w2.shape, w2.dtype),
            pltpu.VMEM((width, 8 * lanes), jnp.bfloat16),
            pltpu.SemaphoreType.DMA((1 + 2 * TILES,)),
        ],
        compiler_params=pltpu.CompilerParams(vmem_limit_bytes=58 * 2**20),
        cost_estimate=pl.CostEstimate(
            flops=8 * width * width * 8 * lanes, bytes_accessed=12 * 2**20, transcendentals=0
        ),
    )(x, w1, w2)

    out_width = own.shape[1]
    partial = pl.pallas_call(
        third_branch,
        name="third_branch",
        out_shape=jax.ShapeDtypeStruct((out_width, 4 * lanes), jnp.bfloat16),
        in_specs=[pl.BlockSpec(memory_space=pltpu.SMEM)] + [vmem] * 5,
        out_specs=vmem,
        compiler_params=pltpu.CompilerParams(vmem_limit_bytes=24 * 2**20),
        cost_estimate=pl.CostEstimate(
            flops=16 * out_width * half * 4 * lanes, bytes_accessed=7 * 2**20, transcendentals=0
        ),
    )(jnp.stack([k2, k0]).astype(jnp.int32), wa, wb, wc, wd, values)

    pieces = lax.all_to_all(partial, "modes", split_axis=0, concat_axis=0, tiled=True)
    mine = out_width // groups
    pieces = pieces.reshape(2, 2, rest, 2, mine, 2, 2, lanes).astype(jnp.float32)
    summed = jnp.sum(pieces, axis=(0, 2)).astype(jnp.bfloat16)
    return summed.transpose(2, 3, 4, 1, 0, 5).reshape(mine, 2, 2, 2, 2 * lanes)


def spread(order, which, start, onehot):
    rows, width = onehot.shape
    positions = start + lax.broadcasted_iota(jnp.int32, (1, width), 1)
    source = jnp.zeros((1, width), jnp.int32)
    for bit in range(order.shape[1]):
        source += jnp.left_shift(jnp.right_shift(positions, bit) & 1, order[which, bit])
    tile = 256

    @pl.loop(0, rows // tile)
    def _(i):
        at = i * tile + lax.broadcasted_iota(jnp.int32, (tile, width), 0)
        onehot[pl.ds(pl.multiple_of(i * tile, tile), tile), :] = jnp.where(
            at == source, 1.0, 0.0
        ).astype(onehot.dtype)


def turn_first(branch, onehot, w1):
    rows, tile = branch.shape[1], 256
    for t in range(2):

        @pl.loop(0, rows // 2 // tile)
        def _(i):
            to = pl.ds(pl.multiple_of(i * tile, tile), tile)
            at = pl.ds(pl.multiple_of(t * (rows // 2) + i * tile, tile), tile)
            for r in range(2):
                w1[t, r, to, :] = jnp.dot(
                    branch[r, at, :], onehot[...], preferred_element_type=jnp.float32
                ).astype(w1.dtype)


def turn_second(branch, onehot, w2):
    rows, tile = branch.shape[1], 256
    half = rows // 2

    @pl.loop(0, rows // tile)
    def _(i):
        at = pl.ds(pl.multiple_of(i * tile, tile), tile)
        real = jnp.dot(branch[0, at, :], onehot[...], preferred_element_type=jnp.float32)
        real = real.astype(w2.dtype)
        for a in range(2):
            w2[0, a, at, :half] = real[:, a * half : (a + 1) * half]
            w2[1, a, at, half:] = real[:, a * half : (a + 1) * half]
        imag = jnp.dot(branch[1, at, :], onehot[...], preferred_element_type=jnp.float32)
        imag = imag.astype(w2.dtype)
        for a in range(2):
            w2[0, a, at, half:] = -imag[:, a * half : (a + 1) * half]
            w2[1, a, at, :half] = imag[:, a * half : (a + 1) * half]


def joined_branches(w1, w2, w21):
    rows, tile = w2.shape[2], 256
    legs = w1.shape[3]

    @pl.loop(0, rows // tile)
    def _(i):
        at = pl.ds(pl.multiple_of(i * tile, tile), tile)
        for t in range(2):
            first = w1[t].reshape(2 * w1.shape[2], legs)
            for a in range(2):
                lo, hi = a * legs, (2 + a) * legs
                real = jnp.dot(w2[0, a, at, :], first, preferred_element_type=jnp.float32)
                real = real.astype(w21.dtype)
                w21[t, 0, at, lo : lo + legs] = real
                w21[t, 1, at, hi : hi + legs] = real
                imag = jnp.dot(w2[1, a, at, :], first, preferred_element_type=jnp.float32)
                imag = imag.astype(w21.dtype)
                w21[t, 0, at, hi : hi + legs] = -imag
                w21[t, 1, at, lo : lo + legs] = imag


def blocks(w):
    rows = w.shape[1] * w.shape[2]
    real = w[0].astype(jnp.float32).reshape(rows, w.shape[3])
    imag = w[1].astype(jnp.float32).reshape(rows, w.shape[3])
    return jnp.concatenate(
        [jnp.concatenate([real, -imag], axis=1), jnp.concatenate([imag, real], axis=1)], axis=0
    ).astype(w.dtype)


def contraction(
    order, pick, stem, b1, b2, w3, out,
    xin, turned_x, cut, x, raw1, raw2, onehot, w1, w2, w21, y2, raw3, own3, relay3, cross3, acc,
    keeps, sends, gots, load_sem, x_send, x_recv, r_send, r_recv, c_send, c_recv, s_send, s_recv,
):
    part, me = lax.axis_index("parts"), lax.axis_index("modes")
    n = lax.axis_size("modes")
    half = n // 2
    quarter = n // 4
    within = me % half
    top = me // half
    second = (me // quarter) % 2
    m_high, m_low, d = within // 4, (within // 2) % 2, within % 2
    inner = top != second
    f32 = jnp.float32
    depth = (n // 2).bit_length()

    def device(index):
        return (part, index)

    def flipped(width):
        return me + width * (1 - 2 * ((me // width) % 2))

    tops = stem.shape[3]
    loads = [pltpu.make_async_copy(w3, raw3, load_sem.at[0])]
    for i in range(tops):
        which = (m_high + tops - 1 - i) % tops
        loads.append(
            pltpu.make_async_copy(stem.at[:, :, :, which], xin.at[i], load_sem.at[1 + i])
        )
    loads.append(pltpu.make_async_copy(b1, raw1, load_sem.at[1 + tops]))
    loads.append(pltpu.make_async_copy(b2, raw2, load_sem.at[2 + tops]))
    for load in loads:
        load.start()
    barrier = pltpu.get_barrier_semaphore()
    across = (1 - top) * half + (1 - second) * quarter + me % quarter
    opposite = (1 - top) * half + within
    beside = top * half + (1 - second) * quarter + me % quarter
    peers = [top * half + (within + i) % half for i in range(1, half)] + [across, opposite]
    for peer in peers:
        pl.semaphore_signal(barrier, inc=1, device_id=device(peer), device_id_type=MESH)

    chunk = raw3.shape[3] // CHUNKS
    loads[0].wait()
    mine = pick[me]
    for k in range(CHUNKS):
        value = raw3[0, :, :, k * chunk : (k + 1) * chunk, :]
        for j in range(1, raw3.shape[0]):
            value = jnp.where(mine == j, raw3[j, :, :, k * chunk : (k + 1) * chunk, :], value)
        own3[k] = value

    def to_relay(k):
        return pltpu.make_async_remote_copy(
            own3.at[k], relay3.at[k], r_send.at[k], r_recv.at[k],
            device_id=device(across), device_id_type=MESH,
        )

    def to_cross(k, r, source, target):
        return pltpu.make_async_remote_copy(
            source.at[k, r], cross3.at[k, r], c_send.at[k, r], c_recv.at[k, r],
            device_id=device(target), device_id_type=MESH,
        )

    def send_third(k, r):
        @pl.when(inner)
        def _():
            if r == 0:
                to_relay(k).wait()
            to_cross(k, r, relay3, beside).start()

        @pl.when(jnp.logical_not(inner))
        def _():
            to_cross(k, r, own3, opposite).start()

    entries, lanes = stem.shape[1], stem.shape[5]

    def x_copy(target, source):
        return pltpu.make_async_remote_copy(
            cut.at[target], x.at[:, :, source], x_send.at[target], x_recv.at[source],
            device_id=device(top * half + target), device_id_type=MESH,
        )

    def piece(z, low, e):
        return (z * 2 + low) * 2 + e

    for i in range(tops):
        loads[1 + i].wait()
        which = (m_high + tops - 1 - i) % tops
        for r in range(2):
            for a in range(2):
                for q in range(lanes // 128):
                    tmp = turned_x.at[(a * 2 + q) % turned_x.shape[0]]
                    tmp[...] = (
                        xin[i, r, :, a, :, q * 128 : (q + 1) * 128]
                        .astype(f32)
                        .reshape(entries * 8, 128)
                    )
                    for row in range(8):
                        low, b, e = row // 4, (row // 2) % 2, row % 2
                        at = b * lanes + q * 128
                        cut[piece(which, low, e), r, a, :, at : at + 128] = tmp[
                            pl.ds(row, entries, stride=8), :
                        ].astype(cut.dtype)
    pl.semaphore_wait(barrier, len(peers))

    @pl.when(inner)
    def _():
        for k in range(CHUNKS):
            to_relay(k).start()

    for i in range(tops):
        which = (m_high + tops - 1 - i) % tops
        for low in range(2):
            for e in range(2):
                if i < tops - 1 or low == 0 or e == 0:
                    target = piece(which, (m_low + 1 - low) % 2, (d + 1 - e) % 2)
                    x_copy(target, within).start()
    x[:, :, within] = cut[within]

    loads[1 + tops].wait()
    legs = w1.shape[3]
    spread(order, 0, top * legs, onehot.at[:, :legs])
    turn_first(raw1, onehot.at[:, :legs], w1)
    loads[2 + tops].wait()
    spread(order, 1, 0, onehot)
    turn_second(raw2, onehot, w2)
    joined_branches(w1, w2, w21)

    for step in range(1, half):
        x_copy((within + step) % half, within).wait_send()

    ahead = [(k, r) for k in range(CHUNKS) for r in range(2)]
    for _ in range(4):
        send_third(*ahead.pop(0))

    for step in range(1, half):
        source = (within + step) % half
        x_copy(source, source).wait_recv()

    tile, columns = 256, x.shape[4]

    @pl.loop(0, legs // tile)
    def _(i):
        values = x[...].reshape(4 * legs, columns)
        for u in range(2):
            rows = pl.ds(pl.multiple_of(u * legs + i * tile, tile), tile)
            to = pl.ds(pl.multiple_of(i * tile, tile), tile)
            for t in range(2):
                for r in range(2):
                    y2[(t + top) % 2, r, to, u * columns : (u + 1) * columns] = jnp.dot(
                        w21[t, r, rows, :], values, preferred_element_type=f32
                    ).astype(y2.dtype)

    def applied(w, t):
        return jnp.dot(
            blocks(w), y2[t].reshape(2 * legs, 2 * columns), preferred_element_type=f32
        )

    widths = [1 << s for s in range(depth)]
    swapped = widths[:1] + widths[1:-1][::-1] + widths[-1:]

    def order_of(u, k):
        return widths

    def exchange(u, stage, k):
        return pltpu.make_async_remote_copy(
            sends[stage].at[u, k], gots[stage].at[u, k],
            s_send.at[u, stage, k], s_recv.at[u, stage, k],
            device_id=device(flipped(order_of(u, k)[stage])), device_id_type=MESH,
        )

    def split(u, stage, k, total):
        width = order_of(u, k)[stage]
        left = sorted(order_of(u, k)[stage:], reverse=True)
        axis = 1 + left.index(width)
        pairs = total.reshape((2,) + (2,) * len(left) + (chunk, columns))
        pick_of = (slice(None),) * axis
        zero, one = pairs[pick_of + (0,)], pairs[pick_of + (1,)]
        bit = (me // width) % 2
        shape = keeps[stage].shape[2:]
        keeps[stage][u, k] = jnp.where(bit == 0, zero, one).reshape(shape)
        sends[stage][u, k] = jnp.where(bit == 0, one, zero).reshape(shape).astype(
            sends[stage].dtype
        )
        exchange(u, stage, k).start()

    def advance(stage, k):
        for u in range(2):
            exchange(u, stage - 1, k).wait_recv()
            total = keeps[stage - 1][u, k] + gots[stage - 1][u, k].astype(f32)
            if stage < depth:
                split(u, stage, k, total)
            else:
                out[:, k * chunk : (k + 1) * chunk, u * columns : (u + 1) * columns] = total[
                    :, 0
                ].astype(out.dtype)

    for step in range(CHUNKS + depth):
        if step < CHUNKS:
            acc[...] = applied(own3.at[step], 0)
            for r in range(2):
                to_cross(step, r, own3, opposite).wait_recv()
            if ahead:
                send_third(*ahead.pop(0))
            total = acc[...] + applied(cross3.at[step], 1)
            for u in range(2):
                part_of = total[:, u * columns : (u + 1) * columns]
                split(u, 0, step, part_of.reshape(2, n, chunk, columns))
            if ahead:
                send_third(*ahead.pop(0))
        for stage in range(depth, 0, -1):
            k = step - stage + 1
            if 0 <= k < CHUNKS:
                advance(stage, k)

    @pl.when(inner)
    def _():
        for k in range(CHUNKS):
            for r in range(2):
                to_cross(k, r, relay3, beside).wait_send()

    @pl.when(jnp.logical_not(inner))
    def _():
        for k in range(CHUNKS):
            for r in range(2):
                to_cross(k, r, own3, opposite).wait_send()

    for stage in range(depth):
        for k in range(CHUNKS):
            for u in range(2):
                exchange(u, stage, k).wait_send()


def by_halves(stem, branch_one, branch_two, branch_three, leg_orders, slice_pick):
    n = lax.axis_size("modes")
    entries, heads, lanes = stem.shape[2], stem.shape[3], stem.shape[4]
    slices, out_width, depth3 = branch_three.shape[0], branch_three.shape[3], branch_three.shape[4]
    legs = branch_one.shape[1]
    mine, tops = out_width // n, n // 8
    chunk = mine // CHUNKS
    stages = (n // 2).bit_length()
    cut = stem.reshape(2, entries, 2, tops, 8, lanes)
    third = branch_three.reshape(slices, 2, n, mine, depth3)
    bf16, f32 = jnp.bfloat16, jnp.float32
    smem = pl.BlockSpec(memory_space=pltpu.SMEM)
    anyspace = pl.BlockSpec(memory_space=pl.ANY)
    dma = pltpu.SemaphoreType.DMA

    def halving(dtype):
        return [
            pltpu.VMEM((2, CHUNKS, 2, n >> (s + 1), chunk, 2 * lanes), dtype)
            for s in range(stages)
        ]

    out = pl.pallas_call(
        contraction,
        name="contraction",
        out_shape=jax.ShapeDtypeStruct((2, mine, 4 * lanes), bf16),
        in_specs=[smem, smem] + [anyspace] * 4,
        out_specs=pl.BlockSpec(memory_space=pltpu.VMEM),
        scratch_shapes=[
            pltpu.VMEM((tops, 2, entries, 2, 8, lanes), bf16),
            pltpu.VMEM((4, entries * 8, 128), f32),
            pltpu.VMEM((n // 2, 2, 2, entries, 2 * lanes), bf16),
            pltpu.VMEM((2, 2, n // 2, entries, 2 * lanes), bf16),
            pltpu.VMEM(branch_one.shape, bf16),
            pltpu.VMEM(branch_two.shape, bf16),
            pltpu.VMEM((legs, legs), bf16),
            pltpu.VMEM((2, 2, legs // 2, legs // 2), bf16),
            pltpu.VMEM((2, 2, legs, legs), bf16),
            pltpu.VMEM((2, 2, legs, 2 * legs), bf16),
            pltpu.VMEM((2, 2, legs // 2, 4 * lanes), bf16),
            pltpu.VMEM(third.shape, bf16),
            pltpu.VMEM((CHUNKS, 2, n, chunk, depth3), bf16),
            pltpu.VMEM((CHUNKS, 2, n, chunk, depth3), bf16),
            pltpu.VMEM((CHUNKS, 2, n, chunk, depth3), bf16),
            pltpu.VMEM((2 * n * chunk, 4 * lanes), f32),
            halving(f32),
            halving(bf16),
            halving(bf16),
            dma((3 + tops,)),
            dma((n // 2,)),
            dma((n // 2,)),
            dma((CHUNKS,)),
            dma((CHUNKS,)),
            dma((CHUNKS, 2)),
            dma((CHUNKS, 2)),
            dma((2, stages, CHUNKS)),
            dma((2, stages, CHUNKS)),
        ],
        compiler_params=pltpu.CompilerParams(
            collective_id=0, has_side_effects=True, vmem_limit_bytes=62 * 2**20
        ),
    )(leg_orders, slice_pick, cut, branch_one, branch_two, third)
    return out.reshape(2, mine, 2, 2, lanes).transpose(1, 0, 2, 3, 4)


def per_device(stem, branch_one, branch_two, branch_three, leg_orders, slice_pick):
    groups = lax.axis_size("modes")
    whole_tiles = (
        groups & (groups - 1) == 0
        and stem.shape[2] % 16 == 0
        and branch_three.shape[3] % (groups * CHUNKS * 8) == 0
    )
    program = by_halves if whole_tiles else by_columns
    return program(stem, branch_one, branch_two, branch_three, leg_orders, slice_pick)


def solution(mesh):
    in_specs = (
        P(None, "modes", None, None, "parts"),
        P(),
        P(),
        P(None, None, "modes", None, None),
        P(),
        P("parts"),
    )
    out_specs = P(("parts", "modes"), None, None, None, None)
    return jax.shard_map(
        per_device, mesh=mesh, in_specs=in_specs, out_specs=out_specs, check_vma=False
    )
```

```python
import jax
import jax.numpy as jnp
from jax import lax
from jax.experimental import pallas as pl
from jax.experimental.pallas import tpu as pltpu
from jax.sharding import PartitionSpec as P

TILES = 4
CHUNKS = 4
MESH = pl.DeviceIdType.MESH


def turn_columns(order, branch, out, onehot):
    width = branch.shape[1]

    @pl.when(pl.program_id(0) == 0)
    def _():
        positions = lax.broadcasted_iota(jnp.int32, (1, width), 1)
        source = jnp.zeros((1, width), jnp.int32)
        for bit in range(order.shape[0]):
            source += jnp.left_shift(jnp.right_shift(positions, bit) & 1, order[bit])
        rows = lax.broadcasted_iota(jnp.int32, (width, width), 0)
        onehot[...] = jnp.where(rows == source, 1.0, 0.0).astype(onehot.dtype)

    out[...] = jnp.dot(
        branch[...], onehot[...], preferred_element_type=jnp.float32
    ).astype(out.dtype)


def turned(branch, order, name):
    width = branch.shape[2]
    flat = branch.reshape(-1, width)
    tile = flat.shape[0] // 8
    out = pl.pallas_call(
        turn_columns,
        name=name,
        grid=(8,),
        out_shape=jax.ShapeDtypeStruct(flat.shape, flat.dtype),
        in_specs=[
            pl.BlockSpec(memory_space=pltpu.SMEM),
            pl.BlockSpec((tile, width), lambda i: (i, 0)),
        ],
        out_specs=pl.BlockSpec((tile, width), lambda i: (i, 0)),
        scratch_shapes=[pltpu.VMEM((width, width), flat.dtype)],
        compiler_params=pltpu.CompilerParams(vmem_limit_bytes=58 * 2**20),
        cost_estimate=pl.CostEstimate(
            flops=2 * flat.shape[0] * width * width,
            bytes_accessed=4 * flat.size,
            transcendentals=0,
        ),
    )(order, flat)
    return out.reshape(branch.shape)


def complex_tile(w, values):
    half = values.shape[1] // 2
    p = jnp.dot(w[0], values, preferred_element_type=jnp.float32)
    q = jnp.dot(w[1], values, preferred_element_type=jnp.float32)
    real = p[:, :half] - q[:, half:]
    imag = p[:, half:] + q[:, :half]
    return real.astype(jnp.bfloat16), imag.astype(jnp.bfloat16)


def two_branches(x_hbm, w1_hbm, w2_hbm, out, x, w1, w2, mid, sems):
    width = x.shape[0]
    half = width // 2
    tile = width // TILES
    lanes = x.shape[1] // 8
    copies = [pltpu.make_async_copy(x_hbm, x, sems.at[0])]
    for which, (source, target) in enumerate(((w1_hbm, w1), (w2_hbm, w2))):
        for i in range(TILES):
            rows = pl.ds(i * tile, tile)
            copies.append(
                pltpu.make_async_copy(
                    source.at[:, rows, :], target.at[:, rows, :], sems.at[1 + which * TILES + i]
                )
            )
    for copy in copies:
        copy.start()
    copies[0].wait()
    for i in range(TILES):
        copies[1 + i].wait()
        t, c = divmod(i * tile, half)
        parts = complex_tile(w1[:, i * tile : (i + 1) * tile, :], x[...])
        for r in range(2):
            for a in range(2):
                at = (2 * r + t) * 2 * lanes
                mid[a * half + c : a * half + c + tile, at : at + 2 * lanes] = parts[r][
                    :, a * 2 * lanes : (a + 1) * 2 * lanes
                ]
    for i in range(TILES):
        copies[1 + TILES + i].wait()
        u, c = divmod(i * tile, half)
        parts = complex_tile(w2[:, i * tile : (i + 1) * tile, :], mid[...])
        for r in range(2):
            for td in range(4):
                at = (2 * r + u) * lanes
                out[td, c : c + tile, at : at + lanes] = parts[r][:, td * lanes : (td + 1) * lanes]


def third_branch(place, wa, wb, wc, wd, values, out):
    k2 = place[0]
    k0 = place[1]
    half = values.shape[2] // 2
    p = q = None
    for w, t, d in ((wa, k2, k0), (wb, 1 - k2, k0), (wc, k2, 1 - k0), (wd, 1 - k2, 1 - k0)):
        block = values[2 * t + d]
        pp = jnp.dot(w[0], block, preferred_element_type=jnp.float32)
        qq = jnp.dot(w[1], block, preferred_element_type=jnp.float32)
        p = pp if p is None else p + pp
        q = qq if q is None else q + qq
    out[:, :half] = (p[:, :half] - q[:, half:]).astype(out.dtype)
    out[:, half:] = (p[:, half:] + q[:, :half]).astype(out.dtype)


def by_columns(stem, branch_one, branch_two, branch_three, leg_orders, slice_pick):
    groups = lax.axis_size("modes")
    me = lax.axis_index("modes")
    rest = groups // 8
    entries, lanes = stem.shape[2], stem.shape[4] // 2
    k2 = (me // (2 * rest)) % 2
    quarter = me // (2 * rest)
    k0 = me % 2

    cut = stem.reshape(2, entries, 2, 2, rest, 2, 2, 2, lanes)
    cut = cut.transpose(3, 7, 4, 5, 1, 0, 2, 6, 8).reshape(groups, entries, 8 * lanes)
    pick = lax.dynamic_index_in_dim(slice_pick, me, 0, keepdims=False)
    own = lax.dynamic_index_in_dim(branch_three, pick, 0, keepdims=False)[:, 0]
    q = 2 * rest
    middle = [(q + i, 2 * q + i) for i in range(q)]
    middle += [(b, a) for a, b in middle]
    outer = [(i, i ^ q) for i in range(groups)] if q & (q - 1) == 0 else [
        (i, i + q if (i // q) % 2 == 0 else i - q) for i in range(groups)
    ]
    cores = [(i, i ^ 1) for i in range(groups)]
    crossed = lax.ppermute(own, "modes", middle)
    w1 = turned(branch_one, leg_orders[0], "turn_one")
    cut, crossed, w1, branch_two = lax.optimization_barrier((cut, crossed, w1, branch_two))
    arrived = lax.all_to_all(cut, "modes", split_axis=0, concat_axis=0, tiled=True)
    x = arrived.reshape(groups * entries, 8 * lanes)
    w2 = turned(branch_two, leg_orders[1], "turn_two")
    crossed, w2 = lax.optimization_barrier((crossed, w2))
    inner = (quarter == 1) | (quarter == 2)
    wa = jnp.where(inner, crossed, own)
    wb = lax.ppermute(wa, "modes", outer)
    wc = lax.ppermute(wa, "modes", cores)
    wd = lax.ppermute(wb, "modes", cores)

    width = w1.shape[1]
    half = width // 2
    any_spec = pl.BlockSpec(memory_space=pl.ANY)
    vmem = pl.BlockSpec(memory_space=pltpu.VMEM)
    values = pl.pallas_call(
        two_branches,
        name="two_branches",
        out_shape=jax.ShapeDtypeStruct((4, half, 4 * lanes), jnp.bfloat16),
        in_specs=[any_spec] * 3,
        out_specs=vmem,
        scratch_shapes=[
            pltpu.VMEM(x.shape, x.dtype),
            pltpu.VMEM(w1.shape, w1.dtype),
            pltpu.VMEM(w2.shape, w2.dtype),
            pltpu.VMEM((width, 8 * lanes), jnp.bfloat16),
            pltpu.SemaphoreType.DMA((1 + 2 * TILES,)),
        ],
        compiler_params=pltpu.CompilerParams(vmem_limit_bytes=58 * 2**20),
        cost_estimate=pl.CostEstimate(
            flops=8 * width * width * 8 * lanes, bytes_accessed=12 * 2**20, transcendentals=0
        ),
    )(x, w1, w2)

    out_width = own.shape[1]
    partial = pl.pallas_call(
        third_branch,
        name="third_branch",
        out_shape=jax.ShapeDtypeStruct((out_width, 4 * lanes), jnp.bfloat16),
        in_specs=[pl.BlockSpec(memory_space=pltpu.SMEM)] + [vmem] * 5,
        out_specs=vmem,
        compiler_params=pltpu.CompilerParams(vmem_limit_bytes=24 * 2**20),
        cost_estimate=pl.CostEstimate(
            flops=16 * out_width * half * 4 * lanes, bytes_accessed=7 * 2**20, transcendentals=0
        ),
    )(jnp.stack([k2, k0]).astype(jnp.int32), wa, wb, wc, wd, values)

    pieces = lax.all_to_all(partial, "modes", split_axis=0, concat_axis=0, tiled=True)
    mine = out_width // groups
    pieces = pieces.reshape(2, 2, rest, 2, mine, 2, 2, lanes).astype(jnp.float32)
    summed = jnp.sum(pieces, axis=(0, 2)).astype(jnp.bfloat16)
    return summed.transpose(2, 3, 4, 1, 0, 5).reshape(mine, 2, 2, 2, 2 * lanes)


def spread(order, which, start, onehot):
    rows, width = onehot.shape
    positions = start + lax.broadcasted_iota(jnp.int32, (1, width), 1)
    source = jnp.zeros((1, width), jnp.int32)
    for bit in range(order.shape[1]):
        source += jnp.left_shift(jnp.right_shift(positions, bit) & 1, order[which, bit])
    tile = 256

    @pl.loop(0, rows // tile)
    def _(i):
        at = i * tile + lax.broadcasted_iota(jnp.int32, (tile, width), 0)
        onehot[pl.ds(pl.multiple_of(i * tile, tile), tile), :] = jnp.where(
            at == source, 1.0, 0.0
        ).astype(onehot.dtype)


def turn_first(branch, onehot, w1):
    rows, tile = branch.shape[1], 256
    for t in range(2):

        @pl.loop(0, rows // 2 // tile)
        def _(i):
            to = pl.ds(pl.multiple_of(i * tile, tile), tile)
            at = pl.ds(pl.multiple_of(t * (rows // 2) + i * tile, tile), tile)
            for r in range(2):
                w1[t, r, to, :] = jnp.dot(
                    branch[r, at, :], onehot[...], preferred_element_type=jnp.float32
                ).astype(w1.dtype)


def turn_second(branch, onehot, w2):
    rows, tile = branch.shape[1], 256
    half = rows // 2

    @pl.loop(0, rows // tile)
    def _(i):
        at = pl.ds(pl.multiple_of(i * tile, tile), tile)
        real = jnp.dot(branch[0, at, :], onehot[...], preferred_element_type=jnp.float32)
        real = real.astype(w2.dtype)
        for a in range(2):
            w2[0, a, at, :half] = real[:, a * half : (a + 1) * half]
            w2[1, a, at, half:] = real[:, a * half : (a + 1) * half]
        imag = jnp.dot(branch[1, at, :], onehot[...], preferred_element_type=jnp.float32)
        imag = imag.astype(w2.dtype)
        for a in range(2):
            w2[0, a, at, half:] = -imag[:, a * half : (a + 1) * half]
            w2[1, a, at, :half] = imag[:, a * half : (a + 1) * half]


def joined_branches(w1, w2, w21):
    rows, tile = w2.shape[2], 256
    legs = w1.shape[3]

    @pl.loop(0, rows // tile)
    def _(i):
        at = pl.ds(pl.multiple_of(i * tile, tile), tile)
        for t in range(2):
            first = w1[t].reshape(2 * w1.shape[2], legs)
            for a in range(2):
                lo, hi = a * legs, (2 + a) * legs
                real = jnp.dot(w2[0, a, at, :], first, preferred_element_type=jnp.float32)
                real = real.astype(w21.dtype)
                w21[t, 0, at, lo : lo + legs] = real
                w21[t, 1, at, hi : hi + legs] = real
                imag = jnp.dot(w2[1, a, at, :], first, preferred_element_type=jnp.float32)
                imag = imag.astype(w21.dtype)
                w21[t, 0, at, hi : hi + legs] = -imag
                w21[t, 1, at, lo : lo + legs] = imag


def blocks(w):
    rows = w.shape[1] * w.shape[2]
    real = w[0].astype(jnp.float32).reshape(rows, w.shape[3])
    imag = w[1].astype(jnp.float32).reshape(rows, w.shape[3])
    return jnp.concatenate(
        [jnp.concatenate([real, -imag], axis=1), jnp.concatenate([imag, real], axis=1)], axis=0
    ).astype(w.dtype)


def contraction(
    order, pick, stem, b1, b2, w3, out,
    xin, turned_x, cut, x, raw1, raw2, onehot, w1, w2, w21, y2, raw3, own3, relay3, cross3, acc,
    keeps, sends, gots, load_sem, x_send, x_recv, r_send, r_recv, c_send, c_recv, s_send, s_recv,
):
    part, me = lax.axis_index("parts"), lax.axis_index("modes")
    n = lax.axis_size("modes")
    half = n // 2
    quarter = n // 4
    within = me % half
    top = me // half
    second = (me // quarter) % 2
    m_high, m_low, d = within // 4, (within // 2) % 2, within % 2
    inner = top != second
    f32 = jnp.float32
    depth = (n // 2).bit_length()

    def device(index):
        return (part, index)

    def flipped(width):
        return me + width * (1 - 2 * ((me // width) % 2))

    tops = stem.shape[3]
    loads = [pltpu.make_async_copy(w3, raw3, load_sem.at[0])]
    for i in range(tops):
        which = (m_high + tops - 1 - i) % tops
        loads.append(
            pltpu.make_async_copy(stem.at[:, :, :, which], xin.at[i], load_sem.at[1 + i])
        )
    loads.append(pltpu.make_async_copy(b1, raw1, load_sem.at[1 + tops]))
    loads.append(pltpu.make_async_copy(b2, raw2, load_sem.at[2 + tops]))
    for load in loads:
        load.start()
    barrier = pltpu.get_barrier_semaphore()
    across = (1 - top) * half + (1 - second) * quarter + me % quarter
    opposite = (1 - top) * half + within
    beside = top * half + (1 - second) * quarter + me % quarter
    peers = [top * half + (within + i) % half for i in range(1, half)] + [across, opposite]
    for peer in peers:
        pl.semaphore_signal(barrier, inc=1, device_id=device(peer), device_id_type=MESH)

    chunk = raw3.shape[3] // CHUNKS
    loads[0].wait()
    mine = pick[me]
    for k in range(CHUNKS):
        value = raw3[0, :, :, k * chunk : (k + 1) * chunk, :]
        for j in range(1, raw3.shape[0]):
            value = jnp.where(mine == j, raw3[j, :, :, k * chunk : (k + 1) * chunk, :], value)
        own3[k] = value

    def to_relay(k):
        return pltpu.make_async_remote_copy(
            own3.at[k], relay3.at[k], r_send.at[k], r_recv.at[k],
            device_id=device(across), device_id_type=MESH,
        )

    def to_cross(k, r, source, target):
        return pltpu.make_async_remote_copy(
            source.at[k, r], cross3.at[k, r], c_send.at[k, r], c_recv.at[k, r],
            device_id=device(target), device_id_type=MESH,
        )

    def send_third(k, r):
        @pl.when(inner)
        def _():
            if r == 0:
                to_relay(k).wait()
            to_cross(k, r, relay3, beside).start()

        @pl.when(jnp.logical_not(inner))
        def _():
            to_cross(k, r, own3, opposite).start()

    entries, lanes = stem.shape[1], stem.shape[5]

    def x_copy(target, source):
        return pltpu.make_async_remote_copy(
            cut.at[target], x.at[:, :, source], x_send.at[target], x_recv.at[source],
            device_id=device(top * half + target), device_id_type=MESH,
        )

    def piece(z, low, e):
        return (z * 2 + low) * 2 + e

    for i in range(tops):
        loads[1 + i].wait()
        which = (m_high + tops - 1 - i) % tops
        for r in range(2):
            for a in range(2):
                for q in range(lanes // 128):
                    tmp = turned_x.at[(a * 2 + q) % turned_x.shape[0]]
                    tmp[...] = (
                        xin[i, r, :, a, :, q * 128 : (q + 1) * 128]
                        .astype(f32)
                        .reshape(entries * 8, 128)
                    )
                    for row in range(8):
                        low, b, e = row // 4, (row // 2) % 2, row % 2
                        at = b * lanes + q * 128
                        cut[piece(which, low, e), r, a, :, at : at + 128] = tmp[
                            pl.ds(row, entries, stride=8), :
                        ].astype(cut.dtype)
    pl.semaphore_wait(barrier, len(peers))

    @pl.when(inner)
    def _():
        for k in range(CHUNKS):
            to_relay(k).start()

    for i in range(tops):
        which = (m_high + tops - 1 - i) % tops
        for low in range(2):
            for e in range(2):
                if i < tops - 1 or low == 0 or e == 0:
                    target = piece(which, (m_low + 1 - low) % 2, (d + 1 - e) % 2)
                    x_copy(target, within).start()
    x[:, :, within] = cut[within]

    loads[1 + tops].wait()
    legs = w1.shape[3]
    spread(order, 0, top * legs, onehot.at[:, :legs])
    turn_first(raw1, onehot.at[:, :legs], w1)
    loads[2 + tops].wait()
    spread(order, 1, 0, onehot)
    turn_second(raw2, onehot, w2)
    joined_branches(w1, w2, w21)

    for step in range(1, half):
        x_copy((within + step) % half, within).wait_send()

    ahead = [(k, r) for k in range(CHUNKS) for r in range(2)]
    for _ in range(4):
        send_third(*ahead.pop(0))

    for step in range(1, half):
        source = (within + step) % half
        x_copy(source, source).wait_recv()

    tile, columns = 256, x.shape[4]

    @pl.loop(0, legs // tile)
    def _(i):
        values = x[...].reshape(4 * legs, columns)
        for u in range(2):
            rows = pl.ds(pl.multiple_of(u * legs + i * tile, tile), tile)
            to = pl.ds(pl.multiple_of(i * tile, tile), tile)
            for t in range(2):
                for r in range(2):
                    y2[(t + top) % 2, r, to, u * columns : (u + 1) * columns] = jnp.dot(
                        w21[t, r, rows, :], values, preferred_element_type=f32
                    ).astype(y2.dtype)

    def applied(w, t):
        return jnp.dot(
            blocks(w), y2[t].reshape(2 * legs, 2 * columns), preferred_element_type=f32
        )

    widths = [1 << s for s in range(depth)]
    swapped = widths[:1] + widths[1:-1][::-1] + widths[-1:]

    def order_of(u, k):
        return swapped if u == 1 and k == CHUNKS - 1 else widths

    def exchange(u, stage, k):
        return pltpu.make_async_remote_copy(
            sends[stage].at[u, k], gots[stage].at[u, k],
            s_send.at[u, stage, k], s_recv.at[u, stage, k],
            device_id=device(flipped(order_of(u, k)[stage])), device_id_type=MESH,
        )

    def split(u, stage, k, total):
        width = order_of(u, k)[stage]
        left = sorted(order_of(u, k)[stage:], reverse=True)
        axis = 1 + left.index(width)
        pairs = total.reshape((2,) + (2,) * len(left) + (chunk, columns))
        pick_of = (slice(None),) * axis
        zero, one = pairs[pick_of + (0,)], pairs[pick_of + (1,)]
        bit = (me // width) % 2
        shape = keeps[stage].shape[2:]
        keeps[stage][u, k] = jnp.where(bit == 0, zero, one).reshape(shape)
        sends[stage][u, k] = jnp.where(bit == 0, one, zero).reshape(shape).astype(
            sends[stage].dtype
        )
        exchange(u, stage, k).start()

    def advance(stage, k):
        for u in range(2):
            exchange(u, stage - 1, k).wait_recv()
            total = keeps[stage - 1][u, k] + gots[stage - 1][u, k].astype(f32)
            if stage < depth:
                split(u, stage, k, total)
            else:
                for r in range(2):
                    for b in range(2):
                        out[k * chunk : (k + 1) * chunk, r, u, b, :] = total[
                            r, 0, :, b * lanes : (b + 1) * lanes
                        ].astype(out.dtype)

    for step in range(CHUNKS + depth):
        if step < CHUNKS:
            acc[...] = applied(own3.at[step], 0)
            for r in range(2):
                to_cross(step, r, own3, opposite).wait_recv()
            if ahead:
                send_third(*ahead.pop(0))
            total = acc[...] + applied(cross3.at[step], 1)
            for u in range(2):
                part_of = total[:, u * columns : (u + 1) * columns]
                split(u, 0, step, part_of.reshape(2, n, chunk, columns))
        for stage in range(1, depth + 1):
            k = step - stage + 1
            if 0 <= k < CHUNKS:
                advance(stage, k)
        if ahead:
            send_third(*ahead.pop(0))

    @pl.when(inner)
    def _():
        for k in range(CHUNKS):
            for r in range(2):
                to_cross(k, r, relay3, beside).wait_send()

    @pl.when(jnp.logical_not(inner))
    def _():
        for k in range(CHUNKS):
            for r in range(2):
                to_cross(k, r, own3, opposite).wait_send()

    for stage in range(depth):
        for k in range(CHUNKS):
            for u in range(2):
                exchange(u, stage, k).wait_send()


def by_halves(stem, branch_one, branch_two, branch_three, leg_orders, slice_pick):
    n = lax.axis_size("modes")
    entries, heads, lanes = stem.shape[2], stem.shape[3], stem.shape[4]
    slices, out_width, depth3 = branch_three.shape[0], branch_three.shape[3], branch_three.shape[4]
    legs = branch_one.shape[1]
    mine, tops = out_width // n, n // 8
    chunk = mine // CHUNKS
    stages = (n // 2).bit_length()
    cut = stem.reshape(2, entries, 2, tops, 8, lanes)
    third = branch_three.reshape(slices, 2, n, mine, depth3)
    bf16, f32 = jnp.bfloat16, jnp.float32
    smem = pl.BlockSpec(memory_space=pltpu.SMEM)
    anyspace = pl.BlockSpec(memory_space=pl.ANY)
    dma = pltpu.SemaphoreType.DMA

    def halving(dtype):
        return [
            pltpu.VMEM((2, CHUNKS, 2, n >> (s + 1), chunk, 2 * lanes), dtype)
            for s in range(stages)
        ]

    return pl.pallas_call(
        contraction,
        name="contraction",
        out_shape=jax.ShapeDtypeStruct((mine, 2, 2, 2, lanes), bf16),
        in_specs=[smem, smem] + [anyspace] * 4,
        out_specs=pl.BlockSpec(memory_space=pltpu.VMEM),
        scratch_shapes=[
            pltpu.VMEM((tops, 2, entries, 2, 8, lanes), bf16),
            pltpu.VMEM((4, entries * 8, 128), f32),
            pltpu.VMEM((n // 2, 2, 2, entries, 2 * lanes), bf16),
            pltpu.VMEM((2, 2, n // 2, entries, 2 * lanes), bf16),
            pltpu.VMEM(branch_one.shape, bf16),
            pltpu.VMEM(branch_two.shape, bf16),
            pltpu.VMEM((legs, legs), bf16),
            pltpu.VMEM((2, 2, legs // 2, legs // 2), bf16),
            pltpu.VMEM((2, 2, legs, legs), bf16),
            pltpu.VMEM((2, 2, legs, 2 * legs), bf16),
            pltpu.VMEM((2, 2, legs // 2, 4 * lanes), bf16),
            pltpu.VMEM(third.shape, bf16),
            pltpu.VMEM((CHUNKS, 2, n, chunk, depth3), bf16),
            pltpu.VMEM((CHUNKS, 2, n, chunk, depth3), bf16),
            pltpu.VMEM((CHUNKS, 2, n, chunk, depth3), bf16),
            pltpu.VMEM((2 * n * chunk, 4 * lanes), f32),
            halving(f32),
            halving(bf16),
            halving(bf16),
            dma((3 + tops,)),
            dma((n // 2,)),
            dma((n // 2,)),
            dma((CHUNKS,)),
            dma((CHUNKS,)),
            dma((CHUNKS, 2)),
            dma((CHUNKS, 2)),
            dma((2, stages, CHUNKS)),
            dma((2, stages, CHUNKS)),
        ],
        compiler_params=pltpu.CompilerParams(
            collective_id=0, has_side_effects=True, vmem_limit_bytes=62 * 2**20
        ),
    )(leg_orders, slice_pick, cut, branch_one, branch_two, third)


def per_device(stem, branch_one, branch_two, branch_three, leg_orders, slice_pick):
    groups = lax.axis_size("modes")
    whole_tiles = (
        groups & (groups - 1) == 0
        and stem.shape[2] % 16 == 0
        and branch_three.shape[3] % (groups * CHUNKS * 8) == 0
    )
    program = by_halves if whole_tiles else by_columns
    return program(stem, branch_one, branch_two, branch_three, leg_orders, slice_pick)


def solution(mesh):
    in_specs = (
        P(None, "modes", None, None, "parts"),
        P(),
        P(),
        P(None, None, "modes", None, None),
        P(),
        P("parts"),
    )
    out_specs = P(("parts", "modes"), None, None, None, None)
    return jax.shard_map(
        per_device, mesh=mesh, in_specs=in_specs, out_specs=out_specs, check_vma=False
    )
```

```python
import jax
import jax.numpy as jnp
from jax import lax
from jax.experimental import pallas as pl
from jax.experimental.pallas import tpu as pltpu
from jax.sharding import PartitionSpec as P

TILES = 4
CHUNKS = 4
MESH = pl.DeviceIdType.MESH


def turn_columns(order, branch, out, onehot):
    width = branch.shape[1]

    @pl.when(pl.program_id(0) == 0)
    def _():
        positions = lax.broadcasted_iota(jnp.int32, (1, width), 1)
        source = jnp.zeros((1, width), jnp.int32)
        for bit in range(order.shape[0]):
            source += jnp.left_shift(jnp.right_shift(positions, bit) & 1, order[bit])
        rows = lax.broadcasted_iota(jnp.int32, (width, width), 0)
        onehot[...] = jnp.where(rows == source, 1.0, 0.0).astype(onehot.dtype)

    out[...] = jnp.dot(
        branch[...], onehot[...], preferred_element_type=jnp.float32
    ).astype(out.dtype)


def turned(branch, order, name):
    width = branch.shape[2]
    flat = branch.reshape(-1, width)
    tile = flat.shape[0] // 8
    out = pl.pallas_call(
        turn_columns,
        name=name,
        grid=(8,),
        out_shape=jax.ShapeDtypeStruct(flat.shape, flat.dtype),
        in_specs=[
            pl.BlockSpec(memory_space=pltpu.SMEM),
            pl.BlockSpec((tile, width), lambda i: (i, 0)),
        ],
        out_specs=pl.BlockSpec((tile, width), lambda i: (i, 0)),
        scratch_shapes=[pltpu.VMEM((width, width), flat.dtype)],
        compiler_params=pltpu.CompilerParams(vmem_limit_bytes=58 * 2**20),
        cost_estimate=pl.CostEstimate(
            flops=2 * flat.shape[0] * width * width,
            bytes_accessed=4 * flat.size,
            transcendentals=0,
        ),
    )(order, flat)
    return out.reshape(branch.shape)


def complex_tile(w, values):
    half = values.shape[1] // 2
    p = jnp.dot(w[0], values, preferred_element_type=jnp.float32)
    q = jnp.dot(w[1], values, preferred_element_type=jnp.float32)
    real = p[:, :half] - q[:, half:]
    imag = p[:, half:] + q[:, :half]
    return real.astype(jnp.bfloat16), imag.astype(jnp.bfloat16)


def two_branches(x_hbm, w1_hbm, w2_hbm, out, x, w1, w2, mid, sems):
    width = x.shape[0]
    half = width // 2
    tile = width // TILES
    lanes = x.shape[1] // 8
    copies = [pltpu.make_async_copy(x_hbm, x, sems.at[0])]
    for which, (source, target) in enumerate(((w1_hbm, w1), (w2_hbm, w2))):
        for i in range(TILES):
            rows = pl.ds(i * tile, tile)
            copies.append(
                pltpu.make_async_copy(
                    source.at[:, rows, :], target.at[:, rows, :], sems.at[1 + which * TILES + i]
                )
            )
    for copy in copies:
        copy.start()
    copies[0].wait()
    for i in range(TILES):
        copies[1 + i].wait()
        t, c = divmod(i * tile, half)
        parts = complex_tile(w1[:, i * tile : (i + 1) * tile, :], x[...])
        for r in range(2):
            for a in range(2):
                at = (2 * r + t) * 2 * lanes
                mid[a * half + c : a * half + c + tile, at : at + 2 * lanes] = parts[r][
                    :, a * 2 * lanes : (a + 1) * 2 * lanes
                ]
    for i in range(TILES):
        copies[1 + TILES + i].wait()
        u, c = divmod(i * tile, half)
        parts = complex_tile(w2[:, i * tile : (i + 1) * tile, :], mid[...])
        for r in range(2):
            for td in range(4):
                at = (2 * r + u) * lanes
                out[td, c : c + tile, at : at + lanes] = parts[r][:, td * lanes : (td + 1) * lanes]


def third_branch(place, wa, wb, wc, wd, values, out):
    k2 = place[0]
    k0 = place[1]
    half = values.shape[2] // 2
    p = q = None
    for w, t, d in ((wa, k2, k0), (wb, 1 - k2, k0), (wc, k2, 1 - k0), (wd, 1 - k2, 1 - k0)):
        block = values[2 * t + d]
        pp = jnp.dot(w[0], block, preferred_element_type=jnp.float32)
        qq = jnp.dot(w[1], block, preferred_element_type=jnp.float32)
        p = pp if p is None else p + pp
        q = qq if q is None else q + qq
    out[:, :half] = (p[:, :half] - q[:, half:]).astype(out.dtype)
    out[:, half:] = (p[:, half:] + q[:, :half]).astype(out.dtype)


def by_columns(stem, branch_one, branch_two, branch_three, leg_orders, slice_pick):
    groups = lax.axis_size("modes")
    me = lax.axis_index("modes")
    rest = groups // 8
    entries, lanes = stem.shape[2], stem.shape[4] // 2
    k2 = (me // (2 * rest)) % 2
    quarter = me // (2 * rest)
    k0 = me % 2

    cut = stem.reshape(2, entries, 2, 2, rest, 2, 2, 2, lanes)
    cut = cut.transpose(3, 7, 4, 5, 1, 0, 2, 6, 8).reshape(groups, entries, 8 * lanes)
    pick = lax.dynamic_index_in_dim(slice_pick, me, 0, keepdims=False)
    own = lax.dynamic_index_in_dim(branch_three, pick, 0, keepdims=False)[:, 0]
    q = 2 * rest
    middle = [(q + i, 2 * q + i) for i in range(q)]
    middle += [(b, a) for a, b in middle]
    outer = [(i, i ^ q) for i in range(groups)] if q & (q - 1) == 0 else [
        (i, i + q if (i // q) % 2 == 0 else i - q) for i in range(groups)
    ]
    cores = [(i, i ^ 1) for i in range(groups)]
    crossed = lax.ppermute(own, "modes", middle)
    w1 = turned(branch_one, leg_orders[0], "turn_one")
    cut, crossed, w1, branch_two = lax.optimization_barrier((cut, crossed, w1, branch_two))
    arrived = lax.all_to_all(cut, "modes", split_axis=0, concat_axis=0, tiled=True)
    x = arrived.reshape(groups * entries, 8 * lanes)
    w2 = turned(branch_two, leg_orders[1], "turn_two")
    crossed, w2 = lax.optimization_barrier((crossed, w2))
    inner = (quarter == 1) | (quarter == 2)
    wa = jnp.where(inner, crossed, own)
    wb = lax.ppermute(wa, "modes", outer)
    wc = lax.ppermute(wa, "modes", cores)
    wd = lax.ppermute(wb, "modes", cores)

    width = w1.shape[1]
    half = width // 2
    any_spec = pl.BlockSpec(memory_space=pl.ANY)
    vmem = pl.BlockSpec(memory_space=pltpu.VMEM)
    values = pl.pallas_call(
        two_branches,
        name="two_branches",
        out_shape=jax.ShapeDtypeStruct((4, half, 4 * lanes), jnp.bfloat16),
        in_specs=[any_spec] * 3,
        out_specs=vmem,
        scratch_shapes=[
            pltpu.VMEM(x.shape, x.dtype),
            pltpu.VMEM(w1.shape, w1.dtype),
            pltpu.VMEM(w2.shape, w2.dtype),
            pltpu.VMEM((width, 8 * lanes), jnp.bfloat16),
            pltpu.SemaphoreType.DMA((1 + 2 * TILES,)),
        ],
        compiler_params=pltpu.CompilerParams(vmem_limit_bytes=58 * 2**20),
        cost_estimate=pl.CostEstimate(
            flops=8 * width * width * 8 * lanes, bytes_accessed=12 * 2**20, transcendentals=0
        ),
    )(x, w1, w2)

    out_width = own.shape[1]
    partial = pl.pallas_call(
        third_branch,
        name="third_branch",
        out_shape=jax.ShapeDtypeStruct((out_width, 4 * lanes), jnp.bfloat16),
        in_specs=[pl.BlockSpec(memory_space=pltpu.SMEM)] + [vmem] * 5,
        out_specs=vmem,
        compiler_params=pltpu.CompilerParams(vmem_limit_bytes=24 * 2**20),
        cost_estimate=pl.CostEstimate(
            flops=16 * out_width * half * 4 * lanes, bytes_accessed=7 * 2**20, transcendentals=0
        ),
    )(jnp.stack([k2, k0]).astype(jnp.int32), wa, wb, wc, wd, values)

    pieces = lax.all_to_all(partial, "modes", split_axis=0, concat_axis=0, tiled=True)
    mine = out_width // groups
    pieces = pieces.reshape(2, 2, rest, 2, mine, 2, 2, lanes).astype(jnp.float32)
    summed = jnp.sum(pieces, axis=(0, 2)).astype(jnp.bfloat16)
    return summed.transpose(2, 3, 4, 1, 0, 5).reshape(mine, 2, 2, 2, 2 * lanes)


def spread(order, which, start, onehot):
    rows, width = onehot.shape
    positions = start + lax.broadcasted_iota(jnp.int32, (1, width), 1)
    source = jnp.zeros((1, width), jnp.int32)
    for bit in range(order.shape[1]):
        source += jnp.left_shift(jnp.right_shift(positions, bit) & 1, order[which, bit])
    tile = 256

    @pl.loop(0, rows // tile)
    def _(i):
        at = i * tile + lax.broadcasted_iota(jnp.int32, (tile, width), 0)
        onehot[pl.ds(pl.multiple_of(i * tile, tile), tile), :] = jnp.where(
            at == source, 1.0, 0.0
        ).astype(onehot.dtype)


def turn_first(branch, onehot, w1):
    rows, tile = branch.shape[1], 256
    for t in range(2):

        @pl.loop(0, rows // 2 // tile)
        def _(i):
            to = pl.ds(pl.multiple_of(i * tile, tile), tile)
            at = pl.ds(pl.multiple_of(t * (rows // 2) + i * tile, tile), tile)
            for r in range(2):
                w1[t, r, to, :] = jnp.dot(
                    branch[r, at, :], onehot[...], preferred_element_type=jnp.float32
                ).astype(w1.dtype)


def turn_second(branch, onehot, w2):
    rows, tile = branch.shape[1], 256
    half = rows // 2

    @pl.loop(0, rows // tile)
    def _(i):
        at = pl.ds(pl.multiple_of(i * tile, tile), tile)
        real = jnp.dot(branch[0, at, :], onehot[...], preferred_element_type=jnp.float32)
        real = real.astype(w2.dtype)
        for a in range(2):
            w2[0, a, at, :half] = real[:, a * half : (a + 1) * half]
            w2[1, a, at, half:] = real[:, a * half : (a + 1) * half]
        imag = jnp.dot(branch[1, at, :], onehot[...], preferred_element_type=jnp.float32)
        imag = imag.astype(w2.dtype)
        for a in range(2):
            w2[0, a, at, half:] = -imag[:, a * half : (a + 1) * half]
            w2[1, a, at, :half] = imag[:, a * half : (a + 1) * half]


def joined_branches(w1, w2, w21):
    rows, tile = w2.shape[2], 256
    legs = w1.shape[3]

    @pl.loop(0, rows // tile)
    def _(i):
        at = pl.ds(pl.multiple_of(i * tile, tile), tile)
        for t in range(2):
            first = w1[t].reshape(2 * w1.shape[2], legs)
            for a in range(2):
                lo, hi = a * legs, (2 + a) * legs
                real = jnp.dot(w2[0, a, at, :], first, preferred_element_type=jnp.float32)
                real = real.astype(w21.dtype)
                w21[t, 0, at, lo : lo + legs] = real
                w21[t, 1, at, hi : hi + legs] = real
                imag = jnp.dot(w2[1, a, at, :], first, preferred_element_type=jnp.float32)
                imag = imag.astype(w21.dtype)
                w21[t, 0, at, hi : hi + legs] = -imag
                w21[t, 1, at, lo : lo + legs] = imag


def blocks(w):
    rows = w.shape[1] * w.shape[2]
    real = w[0].astype(jnp.float32).reshape(rows, w.shape[3])
    imag = w[1].astype(jnp.float32).reshape(rows, w.shape[3])
    return jnp.concatenate(
        [jnp.concatenate([real, -imag], axis=1), jnp.concatenate([imag, real], axis=1)], axis=0
    ).astype(w.dtype)


def contraction(
    order, pick, stem, b1, b2, w3, out,
    xin, turned_x, cut, x, raw1, raw2, onehot, w1, w2, w21, y2, raw3, own3, relay3, cross3, acc,
    keeps, sends, gots, load_sem, x_send, x_recv, r_send, r_recv, c_send, c_recv, s_send, s_recv,
):
    part, me = lax.axis_index("parts"), lax.axis_index("modes")
    n = lax.axis_size("modes")
    half = n // 2
    quarter = n // 4
    within = me % half
    top = me // half
    second = (me // quarter) % 2
    m_high, m_low, d = within // 4, (within // 2) % 2, within % 2
    inner = top != second
    f32 = jnp.float32
    depth = (n // 2).bit_length()

    def device(index):
        return (part, index)

    def flipped(width):
        return me + width * (1 - 2 * ((me // width) % 2))

    tops = stem.shape[3]
    loads = [pltpu.make_async_copy(w3, raw3, load_sem.at[0])]
    for i in range(tops):
        which = (m_high + tops - 1 - i) % tops
        loads.append(
            pltpu.make_async_copy(stem.at[:, :, :, which], xin.at[i], load_sem.at[1 + i])
        )
    loads.append(pltpu.make_async_copy(b1, raw1, load_sem.at[1 + tops]))
    loads.append(pltpu.make_async_copy(b2, raw2, load_sem.at[2 + tops]))
    for load in loads:
        load.start()
    barrier = pltpu.get_barrier_semaphore()
    across = (1 - top) * half + (1 - second) * quarter + me % quarter
    opposite = (1 - top) * half + within
    beside = top * half + (1 - second) * quarter + me % quarter
    peers = [top * half + (within + i) % half for i in range(1, half)] + [across, opposite]
    for peer in peers:
        pl.semaphore_signal(barrier, inc=1, device_id=device(peer), device_id_type=MESH)

    chunk = raw3.shape[3] // CHUNKS
    loads[0].wait()
    mine = pick[me]
    for k in range(CHUNKS):
        value = raw3[0, :, :, k * chunk : (k + 1) * chunk, :]
        for j in range(1, raw3.shape[0]):
            value = jnp.where(mine == j, raw3[j, :, :, k * chunk : (k + 1) * chunk, :], value)
        own3[k] = value

    def to_relay(k):
        return pltpu.make_async_remote_copy(
            own3.at[k], relay3.at[k], r_send.at[k], r_recv.at[k],
            device_id=device(across), device_id_type=MESH,
        )

    def to_cross(k, r, source, target):
        return pltpu.make_async_remote_copy(
            source.at[k, r], cross3.at[k, r], c_send.at[k, r], c_recv.at[k, r],
            device_id=device(target), device_id_type=MESH,
        )

    def send_third(k, r):
        @pl.when(inner)
        def _():
            if r == 0:
                to_relay(k).wait()
            to_cross(k, r, relay3, beside).start()

        @pl.when(jnp.logical_not(inner))
        def _():
            to_cross(k, r, own3, opposite).start()

    entries, lanes = stem.shape[1], stem.shape[5]

    def x_copy(target, source):
        return pltpu.make_async_remote_copy(
            cut.at[target], x.at[:, :, source], x_send.at[target], x_recv.at[source],
            device_id=device(top * half + target), device_id_type=MESH,
        )

    def piece(z, low, e):
        return (z * 2 + low) * 2 + e

    for i in range(tops):
        loads[1 + i].wait()
        which = (m_high + tops - 1 - i) % tops
        for r in range(2):
            for a in range(2):
                for q in range(lanes // 128):
                    tmp = turned_x.at[(a * 2 + q) % turned_x.shape[0]]
                    tmp[...] = (
                        xin[i, r, :, a, :, q * 128 : (q + 1) * 128]
                        .astype(f32)
                        .reshape(entries * 8, 128)
                    )
                    for row in range(8):
                        low, b, e = row // 4, (row // 2) % 2, row % 2
                        at = b * lanes + q * 128
                        cut[piece(which, low, e), r, a, :, at : at + 128] = tmp[
                            pl.ds(row, entries, stride=8), :
                        ].astype(cut.dtype)
    pl.semaphore_wait(barrier, len(peers))

    @pl.when(inner)
    def _():
        for k in range(CHUNKS):
            to_relay(k).start()

    for i in range(tops):
        which = (m_high + tops - 1 - i) % tops
        for low in range(2):
            for e in range(2):
                if i < tops - 1 or low == 0 or e == 0:
                    target = piece(which, (m_low + 1 - low) % 2, (d + 1 - e) % 2)
                    x_copy(target, within).start()
    x[:, :, within] = cut[within]

    loads[1 + tops].wait()
    legs = w1.shape[3]
    spread(order, 0, top * legs, onehot.at[:, :legs])
    turn_first(raw1, onehot.at[:, :legs], w1)
    loads[2 + tops].wait()
    spread(order, 1, 0, onehot)
    turn_second(raw2, onehot, w2)
    joined_branches(w1, w2, w21)

    for step in range(1, half):
        x_copy((within + step) % half, within).wait_send()

    ahead = [(k, r) for k in range(CHUNKS) for r in range(2)]
    for _ in range(4):
        send_third(*ahead.pop(0))

    for step in range(1, half):
        source = (within + step) % half
        x_copy(source, source).wait_recv()

    tile, columns = 256, x.shape[4]

    @pl.loop(0, legs // tile)
    def _(i):
        values = x[...].reshape(4 * legs, columns)
        for u in range(2):
            rows = pl.ds(pl.multiple_of(u * legs + i * tile, tile), tile)
            to = pl.ds(pl.multiple_of(i * tile, tile), tile)
            for t in range(2):
                for r in range(2):
                    y2[(t + top) % 2, r, to, u * columns : (u + 1) * columns] = jnp.dot(
                        w21[t, r, rows, :], values, preferred_element_type=f32
                    ).astype(y2.dtype)

    def applied(w, t):
        return jnp.dot(
            blocks(w), y2[t].reshape(2 * legs, 2 * columns), preferred_element_type=f32
        )

    widths = [1 << s for s in range(depth)]
    swapped = widths[:1] + widths[1:-1][::-1] + widths[-1:]

    def order_of(u, k):
        return swapped if u == 1 and k >= CHUNKS - 2 else widths

    def exchange(u, stage, k):
        return pltpu.make_async_remote_copy(
            sends[stage].at[u, k], gots[stage].at[u, k],
            s_send.at[u, stage, k], s_recv.at[u, stage, k],
            device_id=device(flipped(order_of(u, k)[stage])), device_id_type=MESH,
        )

    def split(u, stage, k, total):
        width = order_of(u, k)[stage]
        left = sorted(order_of(u, k)[stage:], reverse=True)
        axis = 1 + left.index(width)
        pairs = total.reshape((2,) + (2,) * len(left) + (chunk, columns))
        pick_of = (slice(None),) * axis
        zero, one = pairs[pick_of + (0,)], pairs[pick_of + (1,)]
        bit = (me // width) % 2
        shape = keeps[stage].shape[2:]
        keeps[stage][u, k] = jnp.where(bit == 0, zero, one).reshape(shape)
        sends[stage][u, k] = jnp.where(bit == 0, one, zero).reshape(shape).astype(
            sends[stage].dtype
        )
        exchange(u, stage, k).start()

    def advance(stage, k):
        for u in range(2):
            exchange(u, stage - 1, k).wait_recv()
            total = keeps[stage - 1][u, k] + gots[stage - 1][u, k].astype(f32)
            if stage < depth:
                split(u, stage, k, total)
            else:
                for r in range(2):
                    for b in range(2):
                        out[k * chunk : (k + 1) * chunk, r, u, b, :] = total[
                            r, 0, :, b * lanes : (b + 1) * lanes
                        ].astype(out.dtype)

    for step in range(CHUNKS + depth):
        if step < CHUNKS:
            acc[...] = applied(own3.at[step], 0)
            for r in range(2):
                to_cross(step, r, own3, opposite).wait_recv()
            if ahead:
                send_third(*ahead.pop(0))
            total = acc[...] + applied(cross3.at[step], 1)
            for u in range(2):
                part_of = total[:, u * columns : (u + 1) * columns]
                split(u, 0, step, part_of.reshape(2, n, chunk, columns))
        for stage in range(1, depth + 1):
            k = step - stage + 1
            if 0 <= k < CHUNKS:
                advance(stage, k)
        if ahead:
            send_third(*ahead.pop(0))

    @pl.when(inner)
    def _():
        for k in range(CHUNKS):
            for r in range(2):
                to_cross(k, r, relay3, beside).wait_send()

    @pl.when(jnp.logical_not(inner))
    def _():
        for k in range(CHUNKS):
            for r in range(2):
                to_cross(k, r, own3, opposite).wait_send()

    for stage in range(depth):
        for k in range(CHUNKS):
            for u in range(2):
                exchange(u, stage, k).wait_send()


def by_halves(stem, branch_one, branch_two, branch_three, leg_orders, slice_pick):
    n = lax.axis_size("modes")
    entries, heads, lanes = stem.shape[2], stem.shape[3], stem.shape[4]
    slices, out_width, depth3 = branch_three.shape[0], branch_three.shape[3], branch_three.shape[4]
    legs = branch_one.shape[1]
    mine, tops = out_width // n, n // 8
    chunk = mine // CHUNKS
    stages = (n // 2).bit_length()
    cut = stem.reshape(2, entries, 2, tops, 8, lanes)
    third = branch_three.reshape(slices, 2, n, mine, depth3)
    bf16, f32 = jnp.bfloat16, jnp.float32
    smem = pl.BlockSpec(memory_space=pltpu.SMEM)
    anyspace = pl.BlockSpec(memory_space=pl.ANY)
    dma = pltpu.SemaphoreType.DMA

    def halving(dtype):
        return [
            pltpu.VMEM((2, CHUNKS, 2, n >> (s + 1), chunk, 2 * lanes), dtype)
            for s in range(stages)
        ]

    return pl.pallas_call(
        contraction,
        name="contraction",
        out_shape=jax.ShapeDtypeStruct((mine, 2, 2, 2, lanes), bf16),
        in_specs=[smem, smem] + [anyspace] * 4,
        out_specs=pl.BlockSpec(memory_space=pltpu.VMEM),
        scratch_shapes=[
            pltpu.VMEM((tops, 2, entries, 2, 8, lanes), bf16),
            pltpu.VMEM((4, entries * 8, 128), f32),
            pltpu.VMEM((n // 2, 2, 2, entries, 2 * lanes), bf16),
            pltpu.VMEM((2, 2, n // 2, entries, 2 * lanes), bf16),
            pltpu.VMEM(branch_one.shape, bf16),
            pltpu.VMEM(branch_two.shape, bf16),
            pltpu.VMEM((legs, legs), bf16),
            pltpu.VMEM((2, 2, legs // 2, legs // 2), bf16),
            pltpu.VMEM((2, 2, legs, legs), bf16),
            pltpu.VMEM((2, 2, legs, 2 * legs), bf16),
            pltpu.VMEM((2, 2, legs // 2, 4 * lanes), bf16),
            pltpu.VMEM(third.shape, bf16),
            pltpu.VMEM((CHUNKS, 2, n, chunk, depth3), bf16),
            pltpu.VMEM((CHUNKS, 2, n, chunk, depth3), bf16),
            pltpu.VMEM((CHUNKS, 2, n, chunk, depth3), bf16),
            pltpu.VMEM((2 * n * chunk, 4 * lanes), f32),
            halving(f32),
            halving(bf16),
            halving(bf16),
            dma((3 + tops,)),
            dma((n // 2,)),
            dma((n // 2,)),
            dma((CHUNKS,)),
            dma((CHUNKS,)),
            dma((CHUNKS, 2)),
            dma((CHUNKS, 2)),
            dma((2, stages, CHUNKS)),
            dma((2, stages, CHUNKS)),
        ],
        compiler_params=pltpu.CompilerParams(
            collective_id=0, has_side_effects=True, vmem_limit_bytes=62 * 2**20
        ),
    )(leg_orders, slice_pick, cut, branch_one, branch_two, third)


def per_device(stem, branch_one, branch_two, branch_three, leg_orders, slice_pick):
    groups = lax.axis_size("modes")
    whole_tiles = (
        groups & (groups - 1) == 0
        and stem.shape[2] % 16 == 0
        and branch_three.shape[3] % (groups * CHUNKS * 8) == 0
    )
    program = by_halves if whole_tiles else by_columns
    return program(stem, branch_one, branch_two, branch_three, leg_orders, slice_pick)


def solution(mesh):
    in_specs = (
        P(None, "modes", None, None, "parts"),
        P(),
        P(),
        P(None, None, "modes", None, None),
        P(),
        P("parts"),
    )
    out_specs = P(("parts", "modes"), None, None, None, None)
    return jax.shard_map(
        per_device, mesh=mesh, in_specs=in_specs, out_specs=out_specs, check_vma=False
    )
```
